32 devices in a mesh: dp: 4 (over z), ctx: 4 (over y, core), tp: 2 (over x).
Axes of the slice: x: 2, y: 2, z: 4, core: 2. Of those that a mesh axis runs over, the one named last changes fastest.
Arguments:
- queries: bfloat16 [4, 512, 4096], P('dp', 'ctx', 'tp'), may hold values from -8 to 8
- keys_text: bfloat16 [4, 512, 512], P('dp', 'ctx', 'tp'), may hold values from -8 to 8
- values_text: bfloat16 [4, 512, 512], P('dp', 'ctx', 'tp'), may hold values from -6 to 6
- patch_rows: bfloat16 [4, 4, 8, 2, 512], P('dp', 'ctx', None, None, 'tp'), may hold values from -6 to 6
- patch_owner: int32 [4, 4, 8, 1], P('dp', 'ctx'), may hold values from 0 to 3; in each aligned block of 8 rows (0 to 7, 8 to 15, ..., all dimensions but the last counted through in order) at most 4 rows name the same one
- patch_place: int32 [4, 4, 8], P('dp', 'ctx'), may hold values from 0 to 127
- value_head: bfloat16 [4096], P('tp'), may hold values from -0.75 to 0.75
Outputs:
- attention: bfloat16 [4, 512, 4096], P('dp', 'ctx', 'tp')
- value_out: float32 [4, 512], P('dp', 'ctx')
The draws below stay inside these ranges and needn't reach their ends.
Inputs may be any that keep to these rules, and one draw needn't show every extreme that they name: `patch_owner`: among the rows of one vision shard at most 4 name the same sequence, and exactly 4 do in some shards. `patch_place`: rows that share an owner, a ctx index and a position are all added there.
All inputs are finite; a program needn't handle non-finite values.
Results may differ from the reference program's by a relative error of at most 0.0079.
Values may be sent and summed in bfloat16 or wider, within the bound.
A program may use at most 64 MiB of HBM per device.

```python
import math
import jax
import jax.numpy as jnp
import numpy as np
from jax import lax

QHEADS = 32
KVHEADS = 4
HD = 128
TOK_DEV = 128
CAP = 4
LEN = 512
PATCH_DEV = 8
N_DP = 4
N_CTX = 4


def draw_queries(key, part):
    own_key = jax.random.fold_in(key, 11)
    drawn = jnp.clip(jax.random.normal(own_key, (N_DP, LEN, QHEADS * HD), jnp.float32), -8.0, 8.0)
    return drawn.astype(jnp.bfloat16)


def draw_keys_text(key, part):
    own_key = jax.random.fold_in(key, 13)
    drawn = jnp.clip(jax.random.normal(own_key, (N_DP, LEN, KVHEADS * HD), jnp.float32), -8.0, 8.0)
    return drawn.astype(jnp.bfloat16)


def plant(array, key, low, high):
    longest = array.shape.index(max(array.shape))
    spots = []
    for shift in (0, 1):
        where = [jax.random.randint(jax.random.fold_in(key, axis), (), 0, length) for axis, length in enumerate(array.shape)]
        where[longest] = (where[longest] + shift) % array.shape[longest]
        spots.append(tuple(where))
    return array.at[spots[0]].set(low).at[spots[1]].set(high)


def block_levels(rng, dims, pieces, smallest, top_value):
    def one(dim, parts):
        draws = jax.random.uniform(jax.random.fold_in(jax.random.fold_in(rng, 6), dim), (parts,), jnp.float32, smallest / len(pieces), top_value / len(pieces))
        return jnp.repeat(jnp.exp(draws), dims[dim] // parts).reshape((-1,) + (1,) * (len(dims) - dim - 1))

    gain = one(*pieces[0])
    for cut in pieces[1:]:
        gain = gain * one(*cut)
    return gain


def routed_block(key, own, number, rows, count, top, most, lean):
    order = jax.random.permutation(key, count)
    packed, ordinary = shares(count, rows * top, most, lean, True), shares(count, rows * top, most, lean, False)
    places = jnp.arange(count)

    def named(lengths, turn):
        used = int((lengths > 0).sum())
        fixed = max(1, used // 4)
        shifted = fixed + (places - fixed + turn * (used - fixed)) % max(1, count - fixed)
        return jnp.zeros((count,), jnp.int32).at[order[jnp.where(places < fixed, places, shifted)]].set(jnp.asarray(lengths, jnp.int32))

    lengths = jnp.where(number % 4 == 0, named(packed, number // 4), named(ordinary, number - number // 4 - 1))
    mixed = jax.random.permutation(jax.random.fold_in(own, 3), count)
    source_of, receiver = mixed[0:count // 2 * 2:2], mixed[1:count // 2 * 2:2]
    slack = jnp.minimum(lengths[source_of] - 1, most - lengths[receiver]) // 2
    slack = jnp.where((source_of == order[0]) | (receiver == order[0]) | (lengths[receiver] == 0), 0, jnp.maximum(slack, 0))
    shifted = jax.random.randint(jax.random.fold_in(own, 4), (count // 2,), 0, 1 << 20) % (slack + 1)
    lengths = lengths.at[source_of].add(-shifted).at[receiver].add(shifted)
    items = jnp.searchsorted(jnp.cumsum(lengths), jnp.arange(rows * top), side="right").astype(jnp.int32)
    listing = items.reshape(top, rows).T
    listing = listing[jax.random.permutation(jax.random.fold_in(own, 1), rows)]
    turn = jax.random.randint(jax.random.fold_in(own, 2), (rows, 1), 0, top)
    return jnp.take_along_axis(listing, (jnp.arange(top)[None, :] + turn) % top, axis=1)


def shares(amount, total, bound, lean, full):
    portions = [(1 << 20) // math.isqrt(grade ** lean) + 1 for grade in range(1, amount + 1)]
    largest = bound if full else min(bound, max(-(-total // amount), total * portions[0] // sum(portions)))
    least = 1 if total - largest >= amount - 1 else 0
    holding, surplus = [largest] + [least] * (amount - 1), total - largest - least * (amount - 1)
    while surplus > 0:
        movable = [i for i in range(1, amount) if holding[i] < largest] or [i for i in range(1, amount) if holding[i] < bound]
        mass, left = sum([portions[i] for i in movable]), surplus
        for i in movable:
            more = min(bound - holding[i], max(1, left * portions[i] // mass), surplus)
            holding[i] = holding[i] + more
            surplus = surplus - more
    return np.array(holding)


def gaussian(stream_key, extent, scale, reach, cuts=(), kind=jnp.bfloat16):
    gain = block_levels(stream_key, extent, cuts, -0.22, 0.18) if cuts else 1.0
    values = jax.random.normal(stream_key, extent, jnp.float32) * scale * gain
    return jnp.minimum(jnp.maximum(values, -reach), reach).astype(kind)


def setup_inputs(seed: int = 0) -> dict:
    key_list = jax.random.split(jax.random.key(seed), 8)
    queries = draw_queries(jax.random.fold_in(key_list[7], 71), 0)
    keys_text = draw_keys_text(jax.random.fold_in(key_list[7], 71), 0)
    values_text = gaussian(key_list[2], (N_DP, LEN, KVHEADS * HD), 1.0, 6.0, ((0, 4), (1, 4), (2, 2)))
    patch_rows = gaussian(key_list[3], (N_DP, N_CTX, PATCH_DEV, 2, KVHEADS * HD), 1.0, 6.0, ((0, 4), (1, 4), (4, 2)))
    patch_owner_keys = jax.random.split(jax.random.fold_in(key_list[4], 1), N_DP * N_CTX * PATCH_DEV // PATCH_DEV)
    patch_owner_turns = jax.random.permutation(jax.random.fold_in(key_list[4], 3), N_DP * N_CTX * PATCH_DEV // PATCH_DEV)
    patch_owner = jax.vmap(lambda own, number: routed_block(jax.random.fold_in(key_list[4], 2), own, number, PATCH_DEV, N_DP, 1, CAP, 2))(patch_owner_keys, patch_owner_turns).reshape((N_DP, N_CTX, PATCH_DEV, 1))
    patch_place = plant(jax.random.randint(key_list[5], (N_DP, N_CTX, PATCH_DEV), 0, TOK_DEV), jax.random.fold_in(key_list[5], 1), 0, TOK_DEV - 1).astype(jnp.int32)
    value_head = gaussian(key_list[6], (QHEADS * HD,), 64 ** -0.5, 0.75, ((0, 2),))
    return dict(queries=queries, keys_text=keys_text, values_text=values_text, patch_rows=patch_rows, patch_owner=patch_owner, patch_place=patch_place, value_head=value_head)


def attend(queries_seq, keys_seq, values_seq):
    length = queries_seq.shape[0]
    groups = keys_seq.shape[1] // HD
    group_size = queries_seq.shape[1] // keys_seq.shape[1]
    score_scale = HD ** -0.5
    query_split = queries_seq.reshape(length, groups, group_size, HD).astype(jnp.float32)
    key_split = keys_seq.reshape(length, groups, HD).astype(jnp.float32)
    value_split = values_seq.reshape(length, groups, HD).astype(jnp.float32)
    block_rows = 512 if length % 512 == 0 else length
    results = []
    for lower in range(0, length, block_rows):
        upper = lower + block_rows
        scores = jnp.einsum("tgrd,sgd->tgrs", query_split[lower:upper], key_split[:upper]) * score_scale
        allowed = jnp.arange(upper, dtype=jnp.int32)[None, :] <= (lower + jnp.arange(block_rows, dtype=jnp.int32))[:, None]
        allowed = allowed[:, None, None, :]
        scores = jnp.where(allowed, scores, -1e30)
        row_max = jnp.max(scores, axis=-1)
        weights = jnp.where(allowed, jnp.exp(scores - row_max[..., None]), 0.0)
        denominator = jnp.sum(weights, axis=-1)
        rounded = weights.astype(jnp.bfloat16).astype(jnp.float32)
        numerator = jnp.einsum("tgrs,sgd->tgrd", rounded, value_split[:upper])
        mixed = numerator / denominator[..., None]
        results.append(mixed.reshape(block_rows, queries_seq.shape[1]).astype(jnp.bfloat16))
    return jnp.concatenate(results, axis=0)


def reference(queries, keys_text, values_text, patch_rows, patch_owner, patch_place, value_head):
    kv_width = keys_text.shape[2]
    owner_seq = patch_owner[..., 0]
    row_place = jnp.arange(N_CTX, dtype=jnp.int32)[None, :, None] * TOK_DEV + patch_place
    flat_index = (owner_seq * LEN + row_place).reshape(-1).astype(jnp.int32)
    key_add = patch_rows[:, :, :, 0, :].reshape(-1, kv_width).astype(jnp.float32)
    value_add = patch_rows[:, :, :, 1, :].reshape(-1, kv_width).astype(jnp.float32)
    merged_keys = keys_text.reshape(-1, kv_width).astype(jnp.float32).at[flat_index].add(key_add)
    merged_values = values_text.reshape(-1, kv_width).astype(jnp.float32).at[flat_index].add(value_add)
    merged_keys = merged_keys.astype(jnp.bfloat16).reshape(N_DP, LEN, kv_width)
    merged_values = merged_values.astype(jnp.bfloat16).reshape(N_DP, LEN, kv_width)

    def per_sequence(triple):
        return attend(triple[0], triple[1], triple[2])

    attention = lax.map(per_sequence, (queries, merged_keys, merged_values))
    value_out = jnp.dot(attention.reshape(-1, attention.shape[2]), value_head, preferred_element_type=jnp.float32)
    return attention, value_out.reshape(N_DP, LEN)
```

```python
import functools
import math

import jax
import jax.numpy as jnp
from jax import lax
from jax.experimental import pallas as pl
from jax.experimental.pallas import tpu as pltpu
from jax.sharding import PartitionSpec as P

HD = 128
CAP = 4
SLOT_BYTES = 8 * 2**20
MESH = pl.DeviceIdType.MESH


def attend_block(
    carried, query_split, query_place, block_keys, block_values, key_place, score_scale
):
    running_max, denominator, numerator = carried
    scores = (
        jnp.einsum("tgrd,sgd->tgrs", query_split, block_keys, preferred_element_type=jnp.float32)
        * score_scale
    )
    allowed = (key_place[None, :] <= query_place[:, None])[:, None, None, :]
    scores = jnp.where(allowed, scores, -1e30)
    new_max = jnp.maximum(running_max, jnp.max(scores, axis=-1))
    weights = jnp.where(allowed, jnp.exp(scores - new_max[..., None]), 0.0)
    shrink = jnp.exp(running_max - new_max)
    denominator = denominator * shrink + jnp.sum(weights, axis=-1)
    numerator = numerator * shrink[..., None] + jnp.einsum(
        "tgrs,sgd->tgrd",
        weights.astype(jnp.bfloat16),
        block_values,
        preferred_element_type=jnp.float32,
    )
    return (new_max, denominator, numerator)


def unchanged(carried):
    return carried


def collective_body(queries, keys_text, values_text, patch_rows, patch_owner, patch_place, value_head):
    token_count = queries.shape[1]
    kv_width = keys_text.shape[2]
    groups = kv_width // HD
    head_count = queries.shape[2] // HD
    group_size = head_count // groups
    score_scale = HD ** (-0.5)
    dp_count = lax.axis_size("dp")
    slot_count = dp_count * CAP
    owner_seq = patch_owner[0, 0, :, 0]
    places = patch_place[0, 0]
    owner_hits = (owner_seq[:, None] == jnp.arange(dp_count, dtype=jnp.int32)[None, :]).astype(
        jnp.int32
    )
    before = jnp.cumsum(owner_hits, axis=0) - owner_hits
    slot_rank = jnp.sum(before * owner_hits, axis=1)
    target = owner_seq * CAP + slot_rank
    select = (jnp.arange(slot_count, dtype=jnp.int32)[:, None] == target[None, :]).astype(jnp.int32)
    row_data = patch_rows[0, 0].reshape(places.shape[0], 2 * kv_width)
    packed = jnp.dot(
        select.astype(jnp.bfloat16), row_data, preferred_element_type=jnp.float32
    ).astype(jnp.bfloat16)
    filled = jnp.sum(select, axis=1)
    slot_place = jnp.sum(select * places[None, :], axis=1) + (1 - filled) * token_count
    packed = packed.reshape(slot_count, 2, kv_width)
    arrived, arrived_place = (
        lax.all_to_all(packed, "dp", split_axis=0, concat_axis=0, tiled=True),
        lax.all_to_all(slot_place, "dp", split_axis=0, concat_axis=0, tiled=True),
    )
    landing = (jnp.arange(token_count, dtype=jnp.int32)[:, None] == arrived_place[None, :]).astype(
        jnp.bfloat16
    )
    arrivals = jnp.dot(
        landing, arrived.reshape(slot_count, 2 * kv_width), preferred_element_type=jnp.float32
    )
    merged_keys = (keys_text[0].astype(jnp.float32) + arrivals[:, :kv_width]).astype(jnp.bfloat16)
    merged_values = (values_text[0].astype(jnp.float32) + arrivals[:, kv_width:]).astype(
        jnp.bfloat16
    )
    query_split = queries[0].reshape(token_count, groups, group_size, HD)
    first_row = lax.axis_index("ctx") * token_count
    query_place = first_row + jnp.arange(token_count, dtype=jnp.int32)
    initial = (
        jnp.full((token_count, groups, group_size), -1e30, jnp.float32),
        jnp.zeros((token_count, groups, group_size), jnp.float32),
        jnp.zeros((token_count, groups, group_size, HD), jnp.float32),
    )
    carried = initial
    start_row = jnp.int32(0)
    piece_keys = lax.all_gather(merged_keys, "ctx", axis=0, tiled=True)
    piece_values = lax.all_gather(merged_values, "ctx", axis=0, tiled=True)
    piece_rows = piece_keys.shape[0]
    block_rows = min(512, piece_rows)
    for lower in range(0, piece_rows, block_rows):
        upper = min(lower + block_rows, piece_rows)
        block_keys = piece_keys[lower:upper].reshape(upper - lower, groups, HD)
        block_values = piece_values[lower:upper].reshape(upper - lower, groups, HD)
        key_place = start_row + lower + jnp.arange(upper - lower, dtype=jnp.int32)

        def update(state_in):
            return attend_block(
                state_in, query_split, query_place, block_keys, block_values, key_place, score_scale
            )

        carried = lax.cond(
            start_row + lower <= first_row + token_count - 1, update, unchanged, carried
        )
    running_max, denominator, numerator = carried
    attention = (
        (numerator / denominator[..., None])
        .reshape(token_count, head_count * HD)
        .astype(jnp.bfloat16)
    )
    partial_value = jnp.dot(attention, value_head, preferred_element_type=jnp.float32)
    value_out = lax.psum(partial_value, "tp")
    return (attention[None], value_out[None])


def attend_rows(queries, merged_keys, merged_values, probe, out, heads, group, last, token_count):
    group_size = heads // merged_keys.shape[0]
    first = group * group_size
    length = (last + 1) * token_count
    rows = math.gcd(token_count, 32)
    score_scale = HD ** (-0.5) * math.log2(math.e)
    block_keys = merged_keys[group, 0:length, :]
    block_values = merged_values[group, 0:length, :]
    places = [
        pl.ds(pl.multiple_of((first + extra) * HD, HD), HD) for extra in range(group_size)
    ]
    totals = []
    for lower in range(0, token_count, rows):
        span = slice(lower, lower + rows)
        stacked = jnp.concatenate([queries[span, place] for place in places], axis=0)
        scores = lax.dot_general(
            stacked, block_keys, (((1,), (1,)), ((), ())), preferred_element_type=jnp.float32
        )
        row = lower + lax.broadcasted_iota(jnp.int32, (rows, token_count), 0)
        col = lax.broadcasted_iota(jnp.int32, (rows, token_count), 1)
        allowed = jnp.concatenate([col <= row] * group_size, axis=0)
        parts = [scores[:, j * token_count : (j + 1) * token_count] for j in range(last + 1)]
        parts[last] = jnp.where(allowed, parts[last], -1e30)
        top = jnp.max(functools.reduce(jnp.maximum, parts), axis=1, keepdims=True)
        weights = [jnp.exp2((part - top) * score_scale) for part in parts]
        rounded = jnp.concatenate([w.astype(jnp.bfloat16) for w in weights], axis=1)
        sums = jnp.dot(rounded, block_values, preferred_element_type=jnp.float32)
        result = (sums[:, :HD] * (1.0 / sums[:, HD:])).astype(jnp.bfloat16)
        total = jnp.zeros((rows, HD), jnp.float32)
        for extra in range(group_size):
            piece = result[extra * rows : (extra + 1) * rows]
            out[span, places[extra]] = piece
            total = total + piece.astype(jnp.float32) * probe[pl.ds(first + extra, 1), :]
        totals.append(total)
    return jnp.concatenate(totals, axis=0)


def fused_kernel(
    sizes,
    owner_hbm,
    place_hbm,
    rows_hbm,
    keys_hbm,
    values_hbm,
    probe_hbm,
    queries_hbm,
    out_any,
    value_ref,
    queries,
    out,
    text,
    rows_in,
    spots_in,
    merged_keys,
    merged_values,
    probe_raw,
    probe,
    partial,
    partial_in,
    query_sem,
    out_sem,
    local_sem,
    text_send,
    text_recv,
    relay_send,
    patch_send,
    patch_recv,
    pass_send,
    pass_recv,
    value_send,
    value_recv,
):
    dp_count, ctx_count, tp_count = sizes
    d, c, t = lax.axis_index("dp"), lax.axis_index("ctx"), lax.axis_index("tp")
    token_count, kv_width = keys_hbm.shape
    groups = kv_width // HD
    heads = queries.shape[1] // HD
    chips = ctx_count // 2
    side = lax.rem(c, 2)
    chip = c // 2
    partner = c + 1 - 2 * side

    barrier = pltpu.get_barrier_semaphore()

    def greet(device):
        pl.semaphore_signal(barrier, inc=1, device_id=device, device_id_type=MESH)

    greet((d, partner, t))
    for k in range(dp_count):
        for m in range(chips):
            if k or m:
                greet((lax.rem(d + k, dp_count), lax.rem(c + 2 * m, ctx_count), t))
    for k in range(1, tp_count):
        greet((d, c, lax.rem(t + k, tp_count)))
    greetings = dp_count * chips + tp_count - 1

    def lanes(group):
        return slice(group * HD, (group + 1) * HD)

    sources = [
        (rows_hbm, rows_in.at[c, d]),
        (owner_hbm, spots_in.at[c, d, 0]),
        (place_hbm, spots_in.at[c, d, 1]),
        (probe_hbm, probe_raw),
    ]
    for group in range(groups):
        sources.append((keys_hbm.at[:, lanes(group)], text.at[c, group, 0]))
        sources.append((values_hbm.at[:, lanes(group)], text.at[c, group, 1]))
    loads = [
        pltpu.make_async_copy(src, dst, local_sem.at[number])
        for number, (src, dst) in enumerate(sources)
    ]
    load_queries = pltpu.make_async_copy(queries_hbm, queries, query_sem)
    for load in loads:
        load.start()
    load_queries.start()
    merged_values[:, :, HD:] = jnp.ones(
        (groups, ctx_count * token_count, HD), jnp.bfloat16
    )
    with jax.named_scope("w_loads"):
        for load in loads:
            load.wait()
    probe[...] = probe_raw[...].astype(jnp.float32)
    with jax.named_scope("w_barrier"):
        pl.semaphore_wait(barrier, greetings)

    parts = (rows_in, spots_in)

    def patch_copies(k, m):
        there = lax.rem(d + k, dp_count)
        later = c if m == 0 else 2 * m + side
        return [
            pltpu.make_async_remote_copy(
                src_ref=part.at[c, d],
                dst_ref=part.at[c, d],
                send_sem=patch_send.at[k, m, kind],
                recv_sem=patch_recv.at[c, d, kind],
                device_id=(there, later, t),
                device_id_type=MESH,
            )
            for kind, part in enumerate(parts)
        ]

    def for_patches(act):
        for k in range(1, dp_count):
            for copy in patch_copies(k, 0):
                act(copy)
        for k in range(dp_count):
            for m in range(1, chips):

                @pl.when(chip < m)
                def _():
                    for copy in patch_copies(k, m):
                        act(copy)

    def pass_copies(block):
        return [
            pltpu.make_async_remote_copy(
                src_ref=part.at[block],
                dst_ref=part.at[block],
                send_sem=pass_send.at[block, kind],
                recv_sem=pass_recv.at[block, kind],
                device_id=(d, partner, t),
                device_id_type=MESH,
            )
            for kind, part in enumerate(parts)
        ]

    def text_copy(m, group):
        return pltpu.make_async_remote_copy(
            src_ref=text.at[c, group],
            dst_ref=text.at[c, group],
            send_sem=text_send.at[m, group],
            recv_sem=text_recv.at[c, group],
            device_id=(d, 2 * m + side, t),
            device_id_type=MESH,
        )

    def relay_copy(block, group):
        return pltpu.make_async_remote_copy(
            src_ref=text.at[block, group],
            dst_ref=text.at[block, group],
            send_sem=relay_send.at[block, group],
            recv_sem=text_recv.at[block, group],
            device_id=(d, partner, t),
            device_id_type=MESH,
        )

    def for_text(act):
        for group in range(groups):
            for m in range(1, chips):

                @pl.when(chip < m)
                def _():
                    act(text_copy(m, group))

    def relays(block):
        return (block < c + 1 - side) & (side == block % 2)

    with jax.named_scope("starts"):
        for_patches(lambda copy: copy.start())
        for_text(lambda copy: copy.start())

    def wait_patches(block):
        for k in range(1, dp_count):
            there = lax.rem(d + k, dp_count)
            for kind, part in enumerate(parts):
                pltpu.make_async_remote_copy(
                    src_ref=part.at[block, there],
                    dst_ref=part.at[block, there],
                    send_sem=patch_send.at[k, 0, kind],
                    recv_sem=patch_recv.at[block, there, kind],
                    device_id=(there, c, t),
                    device_id_type=MESH,
                ).wait_recv()

    def wait_own_patches(block):
        for kind, part in enumerate(parts):
            pltpu.make_async_remote_copy(
                src_ref=part.at[block, d],
                dst_ref=part.at[block, d],
                send_sem=patch_send.at[0, 0, kind],
                recv_sem=patch_recv.at[block, d, kind],
                device_id=(d, partner, t),
                device_id_type=MESH,
            ).wait_recv()

    def merge(block):
        slots = dp_count * rows_hbm.shape[0]
        spots = spots_in[block]
        code = spots[:, 0] * token_count + spots[:, 1]
        code = jnp.concatenate([code[k] for k in range(dp_count)], axis=1)
        here = d * token_count + lax.broadcasted_iota(jnp.int32, (token_count, slots), 0)
        landing = jnp.where(code == here, 1.0, 0.0).astype(jnp.bfloat16)
        rows = rows_in[block].astype(jnp.float32)
        span = pl.ds(block * token_count, token_count)
        for kind in range(2):
            kind_rows = rows[:, :, kind, :].reshape(slots, kv_width).astype(jnp.bfloat16)
            arrivals = jnp.dot(landing, kind_rows, preferred_element_type=jnp.float32)
            for group in range(groups):
                whole = text[block, group, kind].astype(jnp.float32) + arrivals[:, lanes(group)]
                if kind == 0:
                    merged_keys[group, span, :] = whole.astype(jnp.bfloat16)
                else:
                    merged_values[group, span, 0:HD] = whole.astype(jnp.bfloat16)

    with jax.named_scope("patches"):
        for block in range(ctx_count):

            @pl.when((block <= c) & (side == block % 2))
            def _():
                wait_patches(block)

                @pl.when(block < c)
                def _():
                    wait_own_patches(block)

                @pl.when(relays(block))
                def _():
                    for copy in pass_copies(block):
                        copy.start()

    with jax.named_scope("own"):

        @pl.when(side == 0)
        def _():
            for group in range(groups):
                relay_copy(c, group).start()

        for block in range(ctx_count):

            @pl.when(block == c)
            def _():
                merge(block)

    with jax.named_scope("relay"):
        for group in range(groups):
            for block in range(ctx_count - 2):

                @pl.when((block < c - side) & (side == block % 2))
                def _():
                    relay_copy(block, group).wait_recv()
                    relay_copy(block, group).start()

    with jax.named_scope("merges"):
        for block in range(ctx_count - 1):

            @pl.when((block < c) & (side != block % 2))
            def _():
                for copy in pass_copies(block):
                    copy.wait_recv()
                for group in range(groups):
                    relay_copy(block, group).wait_recv()
                merge(block)

            if block < ctx_count - 2:

                @pl.when((block < c) & (side == block % 2))
                def _():
                    merge(block)

    load_queries.wait()

    def out_copy(group):
        width = queries.shape[1] // groups
        place = pl.ds(pl.multiple_of(group * width, width), width)
        return pltpu.make_async_copy(out.at[:, place], out_any.at[:, place], out_sem.at[group])

    def attend(last):
        def step(group, total):
            total = total + attend_rows(
                queries, merged_keys, merged_values, probe, out, heads, group, last, token_count
            )
            out_copy(group).start()
            return total

        total = lax.fori_loop(0, groups, step, jnp.zeros((token_count, HD), jnp.float32))
        partial[...] = jnp.sum(jnp.transpose(total), axis=0, keepdims=True)

    with jax.named_scope("attend"):
        for last in range(ctx_count):

            @pl.when(c == last)
            def _():
                attend(last)

    value_copies = [
        pltpu.make_async_remote_copy(
            src_ref=partial,
            dst_ref=partial_in.at[k - 1],
            send_sem=value_send.at[k - 1],
            recv_sem=value_recv.at[k - 1],
            device_id=(d, c, lax.rem(t + k, tp_count)),
            device_id_type=MESH,
        )
        for k in range(1, tp_count)
    ]
    for copy in value_copies:
        copy.start()
    with jax.named_scope("tail"):
        for_patches(lambda copy: copy.wait_send())
        for_text(lambda copy: copy.wait_send())
        for block in range(ctx_count):

            @pl.when(relays(block))
            def _():
                for copy in pass_copies(block):
                    copy.wait_send()
                for group in range(groups):
                    relay_copy(block, group).wait_send()

        for group in range(groups):
            out_copy(group).wait()
        for copy in value_copies:
            copy.wait()
    whole = partial[...]
    for k in range(1, tp_count):
        whole = whole + partial_in[k - 1]
    value_ref[...] = whole


def write_kernel(attention, value, attention_hbm, value_hbm, sems):
    pieces = sems.shape[0] - 1
    rows = attention.shape[0] // pieces
    copies = [pltpu.make_async_copy(value, value_hbm, sems.at[pieces])]
    for number in range(pieces):
        span = pl.ds(number * rows, rows)
        copies.append(
            pltpu.make_async_copy(
                attention.at[span, :], attention_hbm.at[span, :], sems.at[number]
            )
        )
    for copy in copies:
        copy.start()
    for copy in copies:
        copy.wait()


def fused_body(sizes, queries, keys_text, values_text, patch_rows, patch_owner, patch_place, value_head):
    dp_count, ctx_count, tp_count = sizes
    _, token_count, query_width = queries.shape
    kv_width = keys_text.shape[2]
    row_count = patch_rows.shape[2]
    heads = query_width // HD
    groups = kv_width // HD
    dma = pltpu.SemaphoreType.DMA
    vmem = pl.BlockSpec(memory_space=pltpu.VMEM)
    anywhere = pl.BlockSpec(memory_space=pl.ANY)
    others = max(tp_count - 1, 1)
    inputs = (
        patch_owner[0, 0].reshape(1, row_count),
        patch_place[0],
        patch_rows[0, 0],
        keys_text[0],
        values_text[0],
        value_head.reshape(heads, HD),
        queries[0],
    )
    shapes = (
        jax.ShapeDtypeStruct((token_count, query_width), jnp.bfloat16),
        jax.ShapeDtypeStruct((1, token_count), jnp.float32),
    )
    attention, value_out = pl.pallas_call(
        functools.partial(fused_kernel, sizes),
        out_shape=shapes,
        in_specs=[pl.BlockSpec(memory_space=pltpu.HBM)] * 7,
        out_specs=(anywhere, vmem),
        scratch_shapes=[
            pltpu.VMEM((token_count, query_width), jnp.bfloat16),
            pltpu.VMEM((token_count, query_width), jnp.bfloat16),
            pltpu.VMEM((ctx_count, groups, 2, token_count, HD), jnp.bfloat16),
            pltpu.VMEM((ctx_count, dp_count, row_count, 2, kv_width), jnp.bfloat16),
            pltpu.VMEM((ctx_count, dp_count, 2, 1, row_count), jnp.int32),
            pltpu.VMEM((groups, ctx_count * token_count, HD), jnp.bfloat16),
            pltpu.VMEM((groups, ctx_count * token_count, 2 * HD), jnp.bfloat16),
            pltpu.VMEM((heads, HD), jnp.bfloat16),
            pltpu.VMEM((heads, HD), jnp.float32),
            pltpu.VMEM((1, token_count), jnp.float32),
            pltpu.VMEM((others, 1, token_count), jnp.float32),
            dma,
            dma((groups,)),
            dma((4 + 2 * groups,)),
            dma((ctx_count // 2, groups)),
            dma((ctx_count, groups)),
            dma((ctx_count, groups)),
            dma((dp_count, ctx_count // 2, 2)),
            dma((ctx_count, dp_count, 2)),
            dma((ctx_count, 2)),
            dma((ctx_count, 2)),
            dma((others,)),
            dma((others,)),
        ],
        compiler_params=pltpu.CompilerParams(
            collective_id=0, has_side_effects=True, vmem_limit_bytes=24 * 2**20
        ),
        name="merged_attention",
    )(*(pltpu.with_memory_space_constraint(array, pltpu.HBM) for array in inputs))
    attention, value_out = pl.pallas_call(
        write_kernel,
        out_shape=shapes,
        in_specs=[anywhere] * 2,
        out_specs=(pl.BlockSpec(memory_space=pltpu.HBM),) * 2,
        scratch_shapes=[dma((math.gcd(token_count // 16, 4) + 1,))],
        compiler_params=pltpu.CompilerParams(vmem_limit_bytes=2**20),
        name="write_out",
    )(*(pltpu.with_memory_space_constraint(array, pltpu.VMEM) for array in (attention, value_out)))
    return (attention[None], value_out)


def body(sizes, queries, keys_text, values_text, patch_rows, patch_owner, patch_place, value_head):
    dp_count, ctx_count, _ = sizes
    arriving = dp_count * ctx_count * patch_rows.size * patch_rows.dtype.itemsize
    arrays = (queries, keys_text, values_text, patch_rows, patch_owner, patch_place, value_head)
    if arriving > SLOT_BYTES or ctx_count % 2:
        return collective_body(*arrays)
    return fused_body(sizes, *arrays)


def solution(mesh):
    in_specs = (
        P("dp", "ctx", "tp"),
        P("dp", "ctx", "tp"),
        P("dp", "ctx", "tp"),
        P("dp", "ctx", None, None, "tp"),
        P("dp", "ctx", None, None),
        P("dp", "ctx", None),
        P("tp"),
    )
    out_specs = (P("dp", "ctx", "tp"), P("dp", "ctx"))
    sizes = tuple(mesh.shape[axis] for axis in ("dp", "ctx", "tp"))
    return jax.shard_map(
        functools.partial(body, sizes),
        mesh=mesh,
        in_specs=in_specs,
        out_specs=out_specs,
        check_vma=False,
    )
```

```python
import functools
import math

import jax
import jax.numpy as jnp
from jax import lax
from jax.experimental import pallas as pl
from jax.experimental.pallas import tpu as pltpu
from jax.sharding import PartitionSpec as P

HD = 128
CAP = 4
SLOT_BYTES = 8 * 2**20
MESH = pl.DeviceIdType.MESH


def attend_block(
    carried, query_split, query_place, block_keys, block_values, key_place, score_scale
):
    running_max, denominator, numerator = carried
    scores = (
        jnp.einsum("tgrd,sgd->tgrs", query_split, block_keys, preferred_element_type=jnp.float32)
        * score_scale
    )
    allowed = (key_place[None, :] <= query_place[:, None])[:, None, None, :]
    scores = jnp.where(allowed, scores, -1e30)
    new_max = jnp.maximum(running_max, jnp.max(scores, axis=-1))
    weights = jnp.where(allowed, jnp.exp(scores - new_max[..., None]), 0.0)
    shrink = jnp.exp(running_max - new_max)
    denominator = denominator * shrink + jnp.sum(weights, axis=-1)
    numerator = numerator * shrink[..., None] + jnp.einsum(
        "tgrs,sgd->tgrd",
        weights.astype(jnp.bfloat16),
        block_values,
        preferred_element_type=jnp.float32,
    )
    return (new_max, denominator, numerator)


def unchanged(carried):
    return carried


def collective_body(queries, keys_text, values_text, patch_rows, patch_owner, patch_place, value_head):
    token_count = queries.shape[1]
    kv_width = keys_text.shape[2]
    groups = kv_width // HD
    head_count = queries.shape[2] // HD
    group_size = head_count // groups
    score_scale = HD ** (-0.5)
    dp_count = lax.axis_size("dp")
    slot_count = dp_count * CAP
    owner_seq = patch_owner[0, 0, :, 0]
    places = patch_place[0, 0]
    owner_hits = (owner_seq[:, None] == jnp.arange(dp_count, dtype=jnp.int32)[None, :]).astype(
        jnp.int32
    )
    before = jnp.cumsum(owner_hits, axis=0) - owner_hits
    slot_rank = jnp.sum(before * owner_hits, axis=1)
    target = owner_seq * CAP + slot_rank
    select = (jnp.arange(slot_count, dtype=jnp.int32)[:, None] == target[None, :]).astype(jnp.int32)
    row_data = patch_rows[0, 0].reshape(places.shape[0], 2 * kv_width)
    packed = jnp.dot(
        select.astype(jnp.bfloat16), row_data, preferred_element_type=jnp.float32
    ).astype(jnp.bfloat16)
    filled = jnp.sum(select, axis=1)
    slot_place = jnp.sum(select * places[None, :], axis=1) + (1 - filled) * token_count
    packed = packed.reshape(slot_count, 2, kv_width)
    arrived, arrived_place = (
        lax.all_to_all(packed, "dp", split_axis=0, concat_axis=0, tiled=True),
        lax.all_to_all(slot_place, "dp", split_axis=0, concat_axis=0, tiled=True),
    )
    landing = (jnp.arange(token_count, dtype=jnp.int32)[:, None] == arrived_place[None, :]).astype(
        jnp.bfloat16
    )
    arrivals = jnp.dot(
        landing, arrived.reshape(slot_count, 2 * kv_width), preferred_element_type=jnp.float32
    )
    merged_keys = (keys_text[0].astype(jnp.float32) + arrivals[:, :kv_width]).astype(jnp.bfloat16)
    merged_values = (values_text[0].astype(jnp.float32) + arrivals[:, kv_width:]).astype(
        jnp.bfloat16
    )
    query_split = queries[0].reshape(token_count, groups, group_size, HD)
    first_row = lax.axis_index("ctx") * token_count
    query_place = first_row + jnp.arange(token_count, dtype=jnp.int32)
    initial = (
        jnp.full((token_count, groups, group_size), -1e30, jnp.float32),
        jnp.zeros((token_count, groups, group_size), jnp.float32),
        jnp.zeros((token_count, groups, group_size, HD), jnp.float32),
    )
    carried = initial
    start_row = jnp.int32(0)
    piece_keys = lax.all_gather(merged_keys, "ctx", axis=0, tiled=True)
    piece_values = lax.all_gather(merged_values, "ctx", axis=0, tiled=True)
    piece_rows = piece_keys.shape[0]
    block_rows = min(512, piece_rows)
    for lower in range(0, piece_rows, block_rows):
        upper = min(lower + block_rows, piece_rows)
        block_keys = piece_keys[lower:upper].reshape(upper - lower, groups, HD)
        block_values = piece_values[lower:upper].reshape(upper - lower, groups, HD)
        key_place = start_row + lower + jnp.arange(upper - lower, dtype=jnp.int32)

        def update(state_in):
            return attend_block(
                state_in, query_split, query_place, block_keys, block_values, key_place, score_scale
            )

        carried = lax.cond(
            start_row + lower <= first_row + token_count - 1, update, unchanged, carried
        )
    running_max, denominator, numerator = carried
    attention = (
        (numerator / denominator[..., None])
        .reshape(token_count, head_count * HD)
        .astype(jnp.bfloat16)
    )
    partial_value = jnp.dot(attention, value_head, preferred_element_type=jnp.float32)
    value_out = lax.psum(partial_value, "tp")
    return (attention[None], value_out[None])


def attend_rows(queries, merged_keys, merged_values, probe, out, heads, group, last, token_count):
    group_size = heads // merged_keys.shape[0]
    first = group * group_size
    length = (last + 1) * token_count
    rows = math.gcd(token_count, 32)
    score_scale = HD ** (-0.5) * math.log2(math.e)
    block_keys = merged_keys[group, 0:length, :]
    block_values = merged_values[group, 0:length, :]
    places = [
        pl.ds(pl.multiple_of((first + extra) * HD, HD), HD) for extra in range(group_size)
    ]
    totals = []
    for lower in range(0, token_count, rows):
        span = slice(lower, lower + rows)
        stacked = jnp.concatenate([queries[span, place] for place in places], axis=0)
        scores = lax.dot_general(
            stacked, block_keys, (((1,), (1,)), ((), ())), preferred_element_type=jnp.float32
        )
        row = lower + lax.broadcasted_iota(jnp.int32, (rows, token_count), 0)
        col = lax.broadcasted_iota(jnp.int32, (rows, token_count), 1)
        allowed = jnp.concatenate([col <= row] * group_size, axis=0)
        parts = [scores[:, j * token_count : (j + 1) * token_count] for j in range(last + 1)]
        parts[last] = jnp.where(allowed, parts[last], -1e30)
        top = jnp.max(functools.reduce(jnp.maximum, parts), axis=1, keepdims=True)
        weights = [jnp.exp2((part - top) * score_scale) for part in parts]
        rounded = jnp.concatenate([w.astype(jnp.bfloat16) for w in weights], axis=1)
        sums = jnp.dot(rounded, block_values, preferred_element_type=jnp.float32)
        result = (sums[:, :HD] * (1.0 / sums[:, HD:])).astype(jnp.bfloat16)
        total = jnp.zeros((rows, HD), jnp.float32)
        for extra in range(group_size):
            piece = result[extra * rows : (extra + 1) * rows]
            out[span, places[extra]] = piece
            total = total + piece.astype(jnp.float32) * probe[pl.ds(first + extra, 1), :]
        totals.append(total)
    return jnp.concatenate(totals, axis=0)


def fused_kernel(
    sizes,
    owner_hbm,
    place_hbm,
    rows_hbm,
    keys_hbm,
    values_hbm,
    probe_hbm,
    queries_hbm,
    out_any,
    value_ref,
    queries,
    out,
    text,
    rows_in,
    spots_in,
    merged_keys,
    merged_values,
    probe_raw,
    probe,
    partial,
    partial_in,
    query_sem,
    out_sem,
    local_sem,
    text_send,
    text_recv,
    relay_send,
    patch_send,
    patch_recv,
    value_send,
    value_recv,
    ready,
):
    dp_count, ctx_count, tp_count = sizes
    d, c, t = lax.axis_index("dp"), lax.axis_index("ctx"), lax.axis_index("tp")
    token_count, kv_width = keys_hbm.shape
    row_count = rows_hbm.shape[0]
    groups = kv_width // HD
    heads = queries.shape[1] // HD
    chips = ctx_count // 2
    side = lax.rem(c, 2)
    chip = c // 2

    barrier = pltpu.get_barrier_semaphore()

    def greet(device):
        pl.semaphore_signal(barrier, inc=1, device_id=device, device_id_type=MESH)

    for m in range(1, ctx_count):
        greet((d, lax.rem(c + m, ctx_count), t))
    for k in range(1, tp_count):
        greet((d, c, lax.rem(t + k, tp_count)))

    def greet_above(there, carry):
        for block in range(ctx_count):
            greet((there, block, t))
        return carry

    lax.fori_loop(d + 1, dp_count, greet_above, 0)

    def lanes(group):
        return slice(group * HD, (group + 1) * HD)

    def copy_of(src, dst, sem):
        return pltpu.make_async_copy(src, dst, sem)

    def wait_bytes(ref, sem):
        copy_of(ref, ref, sem).wait()

    own = c * dp_count + d
    load_patches = [
        copy_of(rows_hbm, rows_in.at[own], local_sem.at[0]),
        copy_of(owner_hbm, spots_in.at[own, 0], local_sem.at[1]),
        copy_of(place_hbm, spots_in.at[own, 1], local_sem.at[1]),
    ]
    load_probe = copy_of(probe_hbm, probe_raw, local_sem.at[2])
    load_queries = copy_of(queries_hbm, queries, query_sem)
    for load in load_patches:
        load.start()
    for group in range(groups):
        for kind, source in enumerate((keys_hbm, values_hbm)):
            copy_of(
                source.at[:, lanes(group)], text.at[c, group, kind], text_recv.at[c, group]
            ).start()
    load_probe.start()
    load_queries.start()
    merged_values[:, :, HD:] = jnp.ones((groups, ctx_count * token_count, HD), jnp.bfloat16)
    with jax.named_scope("w_barrier"):
        pl.semaphore_wait(barrier, ctx_count - 1 + tp_count - 1 + d * ctx_count)

    def announce(there, carry):
        def to_block(block, inner):
            pl.semaphore_signal(
                ready.at[d], inc=1, device_id=(there, block, t), device_id_type=MESH
            )
            return inner

        return lax.fori_loop(0, c + 1, to_block, carry)

    lax.fori_loop(0, d, announce, 0)
    with jax.named_scope("w_loads"):
        wait_bytes(rows_in.at[own], local_sem.at[0])
        wait_bytes(spots_in.at[own], local_sem.at[1])

    parts = (rows_in, spots_in)

    def send_patches(there, last_block):
        def to_block(number, carry):
            for kind, part in enumerate(parts):
                pltpu.make_async_remote_copy(
                    src_ref=part.at[own],
                    dst_ref=part.at[own],
                    send_sem=patch_send.at[kind],
                    recv_sem=patch_recv.at[c, kind],
                    device_id=(there, ctx_count - 1 - number, t),
                    device_id_type=MESH,
                ).start()
            return carry

        lax.fori_loop(0, ctx_count - last_block, to_block, 0)

    def send_down(there, carry):
        send_patches(there, c)
        return carry

    with jax.named_scope("down"):
        lax.fori_loop(0, d, send_down, 0)
        send_patches(d, c + 1)
    with jax.named_scope("w_text"):
        for group in range(groups):
            wait_bytes(text.at[c, group], text_recv.at[c, group])

    def text_copy(group, block, there, sem):
        return pltpu.make_async_remote_copy(
            src_ref=text.at[block, group],
            dst_ref=text.at[block, group],
            send_sem=sem,
            recv_sem=text_recv.at[block, group],
            device_id=(d, there, t),
            device_id_type=MESH,
        )

    with jax.named_scope("texts"):
        for group in range(groups):

            def to_chip(m, carry):
                text_copy(group, c, 2 * m + 1, text_send).start()
                return carry

            lax.fori_loop(chip + side, chips, to_chip, 0)
    load_probe.wait()
    probe[...] = probe_raw[...].astype(jnp.float32)

    def send_up(there, carry):
        pl.semaphore_wait(ready.at[there], ctx_count - c)
        send_patches(there, c)
        return carry

    def relay(group):
        def hand_on(block, carry):
            wait_bytes(text.at[block, group], text_recv.at[block, group])
            text_copy(group, block, c - 1, relay_send).start()
            return carry

        lax.fori_loop(0, (c - 1) * side, hand_on, 0)

    split = jnp.maximum(d + 1, dp_count - 1)
    with jax.named_scope("up1"):
        lax.fori_loop(d + 1, split, send_up, 0)
    with jax.named_scope("relay1"):
        relay(0)
    with jax.named_scope("up2"):
        lax.fori_loop(split, dp_count, send_up, 0)
    with jax.named_scope("relay2"):
        for group in range(1, groups):
            relay(group)

    def out_copy(group):
        width = queries.shape[1] // groups
        place = pl.ds(pl.multiple_of(group * width, width), width)
        return copy_of(out.at[:, place], out_any.at[:, place], out_sem)

    def merge(block):
        slots = dp_count * row_count
        span = slice(block * dp_count, (block + 1) * dp_count)
        spots = spots_in[span]
        code = spots[:, 0] * token_count + spots[:, 1]
        code = jnp.concatenate([code[k] for k in range(dp_count)], axis=1)
        here = d * token_count + lax.broadcasted_iota(jnp.int32, (token_count, slots), 0)
        landing = jnp.where(code == here, 1.0, 0.0).astype(jnp.bfloat16)
        rows = rows_in[span].astype(jnp.float32)
        tokens = slice(block * token_count, (block + 1) * token_count)
        for kind in range(2):
            kind_rows = rows[:, :, kind, :].reshape(slots, kv_width).astype(jnp.bfloat16)
            arrivals = jnp.dot(landing, kind_rows, preferred_element_type=jnp.float32)
            for group in range(groups):
                whole = text[block, group, kind].astype(jnp.float32) + arrivals[:, lanes(group)]
                if kind == 0:
                    merged_keys[group, tokens, :] = whole.astype(jnp.bfloat16)
                else:
                    merged_values[group, tokens, 0:HD] = whole.astype(jnp.bfloat16)

    def attend(last):
        with jax.named_scope("w_patch"):
            for block in range(last + 1):
                senders = dp_count if block < last else dp_count - 1
                for kind, part in enumerate(parts):
                    wait_bytes(
                        part.at[pl.ds(block * dp_count, senders)], patch_recv.at[block, kind]
                    )
        with jax.named_scope("w_kv"):
            first = max(last - 1, 0) if last % 2 else 0
            for group in range(groups):
                for block in range(first, last):
                    wait_bytes(text.at[block, group], text_recv.at[block, group])
        with jax.named_scope("merge"):
            for block in range(last + 1):
                merge(block)
        load_queries.wait()

        def step(group, total):
            total = total + attend_rows(
                queries, merged_keys, merged_values, probe, out, heads, group, last, token_count
            )
            out_copy(group).start()
            return total

        with jax.named_scope("attend"):
            total = lax.fori_loop(0, groups, step, jnp.zeros((token_count, HD), jnp.float32))
            partial[...] = jnp.sum(jnp.transpose(total), axis=0, keepdims=True)

    for last in range(ctx_count):

        @pl.when(c == last)
        def _():
            attend(last)

    value_copies = [
        pltpu.make_async_remote_copy(
            src_ref=partial,
            dst_ref=partial_in.at[k - 1],
            send_sem=value_send.at[k - 1],
            recv_sem=value_recv.at[k - 1],
            device_id=(d, c, lax.rem(t + k, tp_count)),
            device_id_type=MESH,
        )
        for k in range(1, tp_count)
    ]
    for copy in value_copies:
        copy.start()
    with jax.named_scope("tail"):
        for last in range(ctx_count):

            @pl.when(c == last)
            def _():
                sent = dp_count * (ctx_count - last) - 1
                if sent:
                    for kind, part in enumerate(parts):
                        wait_bytes(part.at[pl.ds(0, sent)], patch_send.at[kind])
                chips_after = chips - last // 2 - last % 2
                if chips_after:
                    wait_bytes(text.at[pl.ds(0, chips_after)], text_send)
                if last % 2 and last > 1:
                    wait_bytes(text.at[pl.ds(0, last - 1)], relay_send)

        wait_bytes(out, out_sem)
        for copy in value_copies:
            copy.wait()
    whole = partial[...]
    for k in range(1, tp_count):
        whole = whole + partial_in[k - 1]
    value_ref[...] = whole


def write_kernel(attention, value, attention_hbm, value_hbm, sems):
    pieces = sems.shape[0] - 1
    rows = attention.shape[0] // pieces
    copies = [pltpu.make_async_copy(value, value_hbm, sems.at[pieces])]
    for number in range(pieces):
        span = pl.ds(number * rows, rows)
        copies.append(
            pltpu.make_async_copy(
                attention.at[span, :], attention_hbm.at[span, :], sems.at[number]
            )
        )
    for copy in copies:
        copy.start()
    for copy in copies:
        copy.wait()


def fused_body(sizes, queries, keys_text, values_text, patch_rows, patch_owner, patch_place, value_head):
    dp_count, ctx_count, tp_count = sizes
    _, token_count, query_width = queries.shape
    kv_width = keys_text.shape[2]
    row_count = patch_rows.shape[2]
    heads = query_width // HD
    groups = kv_width // HD
    dma = pltpu.SemaphoreType.DMA
    vmem = pl.BlockSpec(memory_space=pltpu.VMEM)
    anywhere = pl.BlockSpec(memory_space=pl.ANY)
    others = max(tp_count - 1, 1)
    inputs = (
        patch_owner[0, 0].reshape(1, row_count),
        patch_place[0],
        patch_rows[0, 0],
        keys_text[0],
        values_text[0],
        value_head.reshape(heads, HD),
        queries[0],
    )
    shapes = (
        jax.ShapeDtypeStruct((token_count, query_width), jnp.bfloat16),
        jax.ShapeDtypeStruct((1, token_count), jnp.float32),
    )
    attention, value_out = pl.pallas_call(
        functools.partial(fused_kernel, sizes),
        out_shape=shapes,
        in_specs=[pl.BlockSpec(memory_space=pltpu.HBM)] * 7,
        out_specs=(anywhere, vmem),
        scratch_shapes=[
            pltpu.VMEM((token_count, query_width), jnp.bfloat16),
            pltpu.VMEM((token_count, query_width), jnp.bfloat16),
            pltpu.VMEM((ctx_count, groups, 2, token_count, HD), jnp.bfloat16),
            pltpu.VMEM((ctx_count * dp_count, row_count, 2, kv_width), jnp.bfloat16),
            pltpu.VMEM((ctx_count * dp_count, 2, 1, row_count), jnp.int32),
            pltpu.VMEM((groups, ctx_count * token_count, HD), jnp.bfloat16),
            pltpu.VMEM((groups, ctx_count * token_count, 2 * HD), jnp.bfloat16),
            pltpu.VMEM((heads, HD), jnp.bfloat16),
            pltpu.VMEM((heads, HD), jnp.float32),
            pltpu.VMEM((1, token_count), jnp.float32),
            pltpu.VMEM((others, 1, token_count), jnp.float32),
            dma,
            dma,
            dma((3,)),
            dma,
            dma((ctx_count, groups)),
            dma,
            dma((2,)),
            dma((ctx_count, 2)),
            dma((others,)),
            dma((others,)),
            pltpu.SemaphoreType.REGULAR((dp_count,)),
        ],
        compiler_params=pltpu.CompilerParams(
            collective_id=0, has_side_effects=True, vmem_limit_bytes=24 * 2**20
        ),
        name="merged_attention",
    )(*(pltpu.with_memory_space_constraint(array, pltpu.HBM) for array in inputs))
    attention, value_out = pl.pallas_call(
        write_kernel,
        out_shape=shapes,
        in_specs=[anywhere] * 2,
        out_specs=(pl.BlockSpec(memory_space=pltpu.HBM),) * 2,
        scratch_shapes=[dma((math.gcd(token_count // 16, 4) + 1,))],
        compiler_params=pltpu.CompilerParams(vmem_limit_bytes=2**20),
        name="write_out",
    )(*(pltpu.with_memory_space_constraint(array, pltpu.VMEM) for array in (attention, value_out)))
    return (attention[None], value_out)


def body(sizes, queries, keys_text, values_text, patch_rows, patch_owner, patch_place, value_head):
    dp_count, ctx_count, _ = sizes
    arriving = dp_count * ctx_count * patch_rows.size * patch_rows.dtype.itemsize
    arrays = (queries, keys_text, values_text, patch_rows, patch_owner, patch_place, value_head)
    if arriving > SLOT_BYTES or ctx_count % 2:
        return collective_body(*arrays)
    return fused_body(sizes, *arrays)


def solution(mesh):
    in_specs = (
        P("dp", "ctx", "tp"),
        P("dp", "ctx", "tp"),
        P("dp", "ctx", "tp"),
        P("dp", "ctx", None, None, "tp"),
        P("dp", "ctx", None, None),
        P("dp", "ctx", None),
        P("tp"),
    )
    out_specs = (P("dp", "ctx", "tp"), P("dp", "ctx"))
    sizes = tuple(mesh.shape[axis] for axis in ("dp", "ctx", "tp"))
    return jax.shard_map(
        functools.partial(body, sizes),
        mesh=mesh,
        in_specs=in_specs,
        out_specs=out_specs,
        check_vma=False,
    )
```

```python
import functools
import math

import jax
import jax.numpy as jnp
from jax import lax
from jax.experimental import pallas as pl
from jax.experimental.pallas import tpu as pltpu
from jax.sharding import PartitionSpec as P

HD = 128
CAP = 4
SLOT_BYTES = 8 * 2**20
MESH = pl.DeviceIdType.MESH


def attend_block(
    carried, query_split, query_place, block_keys, block_values, key_place, score_scale
):
    running_max, denominator, numerator = carried
    scores = (
        jnp.einsum("tgrd,sgd->tgrs", query_split, block_keys, preferred_element_type=jnp.float32)
        * score_scale
    )
    allowed = (key_place[None, :] <= query_place[:, None])[:, None, None, :]
    scores = jnp.where(allowed, scores, -1e30)
    new_max = jnp.maximum(running_max, jnp.max(scores, axis=-1))
    weights = jnp.where(allowed, jnp.exp(scores - new_max[..., None]), 0.0)
    shrink = jnp.exp(running_max - new_max)
    denominator = denominator * shrink + jnp.sum(weights, axis=-1)
    numerator = numerator * shrink[..., None] + jnp.einsum(
        "tgrs,sgd->tgrd",
        weights.astype(jnp.bfloat16),
        block_values,
        preferred_element_type=jnp.float32,
    )
    return (new_max, denominator, numerator)


def unchanged(carried):
    return carried


def collective_body(queries, keys_text, values_text, patch_rows, patch_owner, patch_place, value_head):
    token_count = queries.shape[1]
    kv_width = keys_text.shape[2]
    groups = kv_width // HD
    head_count = queries.shape[2] // HD
    group_size = head_count // groups
    score_scale = HD ** (-0.5)
    dp_count = lax.axis_size("dp")
    slot_count = dp_count * CAP
    owner_seq = patch_owner[0, 0, :, 0]
    places = patch_place[0, 0]
    owner_hits = (owner_seq[:, None] == jnp.arange(dp_count, dtype=jnp.int32)[None, :]).astype(
        jnp.int32
    )
    before = jnp.cumsum(owner_hits, axis=0) - owner_hits
    slot_rank = jnp.sum(before * owner_hits, axis=1)
    target = owner_seq * CAP + slot_rank
    select = (jnp.arange(slot_count, dtype=jnp.int32)[:, None] == target[None, :]).astype(jnp.int32)
    row_data = patch_rows[0, 0].reshape(places.shape[0], 2 * kv_width)
    packed = jnp.dot(
        select.astype(jnp.bfloat16), row_data, preferred_element_type=jnp.float32
    ).astype(jnp.bfloat16)
    filled = jnp.sum(select, axis=1)
    slot_place = jnp.sum(select * places[None, :], axis=1) + (1 - filled) * token_count
    packed = packed.reshape(slot_count, 2, kv_width)
    arrived, arrived_place = (
        lax.all_to_all(packed, "dp", split_axis=0, concat_axis=0, tiled=True),
        lax.all_to_all(slot_place, "dp", split_axis=0, concat_axis=0, tiled=True),
    )
    landing = (jnp.arange(token_count, dtype=jnp.int32)[:, None] == arrived_place[None, :]).astype(
        jnp.bfloat16
    )
    arrivals = jnp.dot(
        landing, arrived.reshape(slot_count, 2 * kv_width), preferred_element_type=jnp.float32
    )
    merged_keys = (keys_text[0].astype(jnp.float32) + arrivals[:, :kv_width]).astype(jnp.bfloat16)
    merged_values = (values_text[0].astype(jnp.float32) + arrivals[:, kv_width:]).astype(
        jnp.bfloat16
    )
    query_split = queries[0].reshape(token_count, groups, group_size, HD)
    first_row = lax.axis_index("ctx") * token_count
    query_place = first_row + jnp.arange(token_count, dtype=jnp.int32)
    initial = (
        jnp.full((token_count, groups, group_size), -1e30, jnp.float32),
        jnp.zeros((token_count, groups, group_size), jnp.float32),
        jnp.zeros((token_count, groups, group_size, HD), jnp.float32),
    )
    carried = initial
    start_row = jnp.int32(0)
    piece_keys = lax.all_gather(merged_keys, "ctx", axis=0, tiled=True)
    piece_values = lax.all_gather(merged_values, "ctx", axis=0, tiled=True)
    piece_rows = piece_keys.shape[0]
    block_rows = min(512, piece_rows)
    for lower in range(0, piece_rows, block_rows):
        upper = min(lower + block_rows, piece_rows)
        block_keys = piece_keys[lower:upper].reshape(upper - lower, groups, HD)
        block_values = piece_values[lower:upper].reshape(upper - lower, groups, HD)
        key_place = start_row + lower + jnp.arange(upper - lower, dtype=jnp.int32)

        def update(state_in):
            return attend_block(
                state_in, query_split, query_place, block_keys, block_values, key_place, score_scale
            )

        carried = lax.cond(
            start_row + lower <= first_row + token_count - 1, update, unchanged, carried
        )
    running_max, denominator, numerator = carried
    attention = (
        (numerator / denominator[..., None])
        .reshape(token_count, head_count * HD)
        .astype(jnp.bfloat16)
    )
    partial_value = jnp.dot(attention, value_head, preferred_element_type=jnp.float32)
    value_out = lax.psum(partial_value, "tp")
    return (attention[None], value_out[None])


def attend(queries, merged_keys, merged_values, probe, out, last, group, totals):
    token_count, width = queries.shape
    groups = merged_keys.shape[0]
    group_size = width // HD // groups
    length = (last + 1) * token_count
    rows = token_count // len(totals)
    score_scale = HD ** (-0.5) * math.log2(math.e)
    heads = range(group * group_size, (group + 1) * group_size)
    block_keys = merged_keys[group, 0:length, :]
    block_values = merged_values[group, 0:length, :]
    for number in range(len(totals)):
        lower = number * rows
        span = slice(lower, lower + rows)
        stacked = jnp.concatenate(
            [queries[span, head * HD : (head + 1) * HD] for head in heads], axis=0
        )
        scores = lax.dot_general(
            stacked, block_keys, (((1,), (1,)), ((), ())), preferred_element_type=jnp.float32
        )
        row = lower + lax.broadcasted_iota(jnp.int32, (rows, token_count), 0)
        col = lax.broadcasted_iota(jnp.int32, (rows, token_count), 1)
        allowed = jnp.concatenate([col <= row] * group_size, axis=0)
        parts = [scores[:, j * token_count : (j + 1) * token_count] for j in range(last + 1)]
        parts[last] = jnp.where(allowed, parts[last], -1e30)
        top = jnp.max(functools.reduce(jnp.maximum, parts), axis=1, keepdims=True)
        weights = [jnp.exp2((part - top) * score_scale) for part in parts]
        rounded = jnp.concatenate([w.astype(jnp.bfloat16) for w in weights], axis=1)
        sums = jnp.dot(rounded, block_values, preferred_element_type=jnp.float32)
        result = (sums[:, :HD] * (1.0 / sums[:, HD:])).astype(jnp.bfloat16)
        for extra, head in enumerate(heads):
            piece = result[extra * rows : (extra + 1) * rows]
            out[span, head * HD : (head + 1) * HD] = piece
            totals[number] = (
                totals[number] + piece.astype(jnp.float32) * probe[head : head + 1, :]
            )


def fused_kernel(
    sizes,
    owner_hbm,
    place_hbm,
    rows_hbm,
    keys_hbm,
    values_hbm,
    probe_hbm,
    queries_hbm,
    out_any,
    value_ref,
    queries,
    out,
    text,
    rows_in,
    spots_in,
    merged_keys,
    merged_values,
    probe_raw,
    probe,
    partial,
    partial_in,
    query_sem,
    out_sem,
    local_sem,
    text_send,
    text_recv,
    relay_send,
    patch_send,
    patch_recv,
    pass_send,
    value_send,
    value_recv,
    ready,
):
    dp_count, ctx_count, tp_count = sizes
    d, c, t = lax.axis_index("dp"), lax.axis_index("ctx"), lax.axis_index("tp")
    token_count, kv_width = keys_hbm.shape
    row_count = rows_hbm.shape[0]
    groups = kv_width // HD
    heads = queries.shape[1] // HD
    chips = ctx_count // 2
    side = lax.rem(c, 2)
    chip = c // 2

    barrier = pltpu.get_barrier_semaphore()
    in_pair = dp_count

    def greet(*device):
        pl.semaphore_signal(barrier, inc=1, device_id=device, device_id_type=MESH)

    def over(lower, upper, act):
        def step(number, carry):
            act(number)
            return carry

        lax.fori_loop(lower, upper, step, 0)

    over(1, ctx_count, lambda step: greet(d, lax.rem(c + step, ctx_count), t))
    over(t + 1, tp_count, lambda other: greet(d, c, other))

    def greet_plane(there):
        for block in range(ctx_count):
            greet(there, block, t)

    over(d + 1, dp_count, greet_plane)

    def lanes(group):
        return slice(group * HD, (group + 1) * HD)

    def copy_of(src, dst, sem):
        return pltpu.make_async_copy(src, dst, sem)

    def wait_bytes(ref, sem):
        copy_of(ref, ref, sem).wait()

    own = c * dp_count + d
    load_patches = [
        copy_of(rows_hbm, rows_in.at[own], local_sem.at[0]),
        copy_of(owner_hbm, spots_in.at[own, 0], local_sem.at[1]),
        copy_of(place_hbm, spots_in.at[own, 1], local_sem.at[1]),
    ]
    load_probe = copy_of(probe_hbm, probe_raw, local_sem.at[2])
    load_queries = copy_of(queries_hbm, queries, query_sem)
    for load in load_patches:
        load.start()
    for group in range(groups):
        for kind, source in enumerate((keys_hbm, values_hbm)):
            copy_of(
                source.at[:, lanes(group)], text.at[c, group, kind], text_recv.at[c, group]
            ).start()
    load_probe.start()
    load_queries.start()
    merged_values[:, :, HD:] = jnp.ones((groups, ctx_count * token_count, HD), jnp.bfloat16)
    with jax.named_scope("w_barrier"):
        pl.semaphore_wait(barrier, d * ctx_count + ctx_count - 1 + t)

    def announce(number, *device):
        pl.semaphore_signal(
            ready.at[number], inc=1, device_id=device, device_id_type=MESH
        )

    over(
        0,
        d,
        lambda there: over(c * side, c + 1, lambda block: announce(d, there, block, t)),
    )
    over(0, t, lambda other: announce(in_pair, d, c, other))
    with jax.named_scope("w_loads"):
        wait_bytes(rows_in.at[own], local_sem.at[0])
        wait_bytes(spots_in.at[own], local_sem.at[1])

    parts = (rows_in, spots_in)

    def send_patches(there, own_block):
        def to_block(block):
            for kind, part in enumerate(parts):
                pltpu.make_async_remote_copy(
                    src_ref=part.at[own],
                    dst_ref=part.at[own],
                    send_sem=patch_send.at[kind],
                    recv_sem=patch_recv.at[c, kind],
                    device_id=(there, block, t),
                    device_id_type=MESH,
                ).start()

        over(0, chips - 1 - chip, lambda number: to_block(2 * (chips - 1 - number)))
        if own_block:
            to_block(c)

    with jax.named_scope("down"):
        over(0, d, lambda there: send_patches(there, True))
    send_patches(d, False)
    with jax.named_scope("w_text"):
        for group in range(groups):
            wait_bytes(text.at[c, group], text_recv.at[c, group])

    def text_copy(group, block, there, sem):
        return pltpu.make_async_remote_copy(
            src_ref=text.at[block, group],
            dst_ref=text.at[block, group],
            send_sem=sem,
            recv_sem=text_recv.at[block, group],
            device_id=(d, there, t),
            device_id_type=MESH,
        )

    with jax.named_scope("texts"):
        for group in range(groups):
            over(
                chip + side,
                chips,
                lambda m: text_copy(group, c, 2 * m + 1, text_send).start(),
            )

    load_probe.wait()
    probe[...] = probe_raw[...].astype(jnp.float32)

    def send_up(there):
        pl.semaphore_wait(ready.at[there], chips - chip)
        send_patches(there, True)

    def relay(group):
        def hand_on(block):
            wait_bytes(text.at[block, group], text_recv.at[block, group])
            text_copy(group, block, c - 1, relay_send).start()

        over(0, (c - 1) * side, hand_on)

    with jax.named_scope("up"):
        over(d + 1, dp_count, send_up)
    with jax.named_scope("relay"):
        for group in range(groups):
            relay(group)

    def pass_patches(block):
        span = pl.ds(block * dp_count, dp_count)
        for kind, part in enumerate(parts):
            pltpu.make_async_remote_copy(
                src_ref=part.at[span],
                dst_ref=part.at[span],
                send_sem=pass_send.at[kind],
                recv_sem=patch_recv.at[block, kind],
                device_id=(d, c + 1, t),
                device_id_type=MESH,
            ).start()

    def merge(block, chosen):
        slots = dp_count * row_count
        span = slice(block * dp_count, (block + 1) * dp_count)
        spots = spots_in[span]
        code = spots[:, 0] * token_count + spots[:, 1]
        code = jnp.concatenate([code[k] for k in range(dp_count)], axis=1)
        here = d * token_count + lax.broadcasted_iota(jnp.int32, (token_count, slots), 0)
        landing = jnp.where(code == here, 1.0, 0.0).astype(jnp.bfloat16)
        wide = slice(chosen[0] * HD, (chosen[-1] + 1) * HD)
        rows = rows_in[span, :, :, wide].astype(jnp.float32)
        tokens = slice(block * token_count, (block + 1) * token_count)
        for kind in range(2):
            kind_rows = rows[:, :, kind, :].reshape(slots, -1).astype(jnp.bfloat16)
            arrivals = jnp.dot(landing, kind_rows, preferred_element_type=jnp.float32)
            for number, group in enumerate(chosen):
                whole = text[block, group, kind].astype(jnp.float32) + arrivals[:, lanes(number)]
                if kind == 0:
                    merged_keys[group, tokens, :] = whole.astype(jnp.bfloat16)
                else:
                    merged_values[group, tokens, 0:HD] = whole.astype(jnp.bfloat16)

    def finish(last):
        with jax.named_scope("w_patch"):
            for block in range(last + 1):
                senders = dp_count if block < last else dp_count - 1
                for kind, part in enumerate(parts):
                    wait_bytes(
                        part.at[pl.ds(block * dp_count, senders)], patch_recv.at[block, kind]
                    )
                if last % 2 == 0:
                    pass_patches(block)
        odd = last % 2
        whole = odd or last == 0
        rows = math.gcd(token_count, 16 if odd else 64)
        totals = [jnp.zeros((rows, HD), jnp.float32)] * (token_count // rows)
        load_queries.wait()

        def compute(chosen):
            for block in range(last + 1):
                merge(block, chosen)
            for group in chosen:
                attend(queries, merged_keys, merged_values, probe, out, last, group, totals)

        for group in range(groups):
            with jax.named_scope("w_kv%d" % group):
                for block in range(last - 1 if odd else 0, last):
                    wait_bytes(text.at[block, group], text_recv.at[block, group])
            if not whole:
                with jax.named_scope("attend%d" % group):
                    compute((group,))
        if whole:
            with jax.named_scope("attend"):
                compute(range(groups))
        total = jnp.concatenate(totals, axis=0)
        partial[...] = jnp.sum(jnp.transpose(total), axis=0, keepdims=True)

    for last in range(ctx_count):

        @pl.when(c == last)
        def _():
            finish(last)

    value_copies = [
        pltpu.make_async_remote_copy(
            src_ref=partial,
            dst_ref=partial_in.at[k - 1],
            send_sem=value_send.at[k - 1],
            recv_sem=value_recv.at[k - 1],
            device_id=(d, c, lax.rem(t + k, tp_count)),
            device_id_type=MESH,
        )
        for k in range(1, tp_count)
    ]
    with jax.named_scope("w_pair"):

        @pl.when(t < tp_count - 1)
        def _():
            pl.semaphore_wait(ready.at[in_pair], tp_count - 1 - t)

    for copy in value_copies:
        copy.start()
    store = copy_of(out, out_any, out_sem)
    store.start()
    with jax.named_scope("tail"):
        for last in range(ctx_count):

            @pl.when(c == last)
            def _():
                later = chips - 1 - last // 2
                sent = dp_count * (later + 1) - 1
                if sent:
                    for kind, part in enumerate(parts):
                        wait_bytes(part.at[pl.ds(0, sent)], patch_send.at[kind])
                copies = later + 1 - last % 2
                if copies:
                    wait_bytes(text.at[pl.ds(0, copies)], text_send)
                if last % 2 and last > 1:
                    wait_bytes(text.at[pl.ds(0, last - 1)], relay_send)
                if last % 2 == 0:
                    for kind, part in enumerate(parts):
                        wait_bytes(part.at[pl.ds(0, (last + 1) * dp_count)], pass_send.at[kind])

        store.wait()
        for copy in value_copies:
            copy.wait()
    whole = partial[...]
    for k in range(1, tp_count):
        whole = whole + partial_in[k - 1]
    value_ref[...] = whole


def write_kernel(attention, value, attention_hbm, value_hbm, sems):
    pieces = sems.shape[0] - 1
    rows = attention.shape[0] // pieces
    copies = [pltpu.make_async_copy(value, value_hbm, sems.at[pieces])]
    for number in range(pieces):
        span = pl.ds(number * rows, rows)
        copies.append(
            pltpu.make_async_copy(
                attention.at[span, :], attention_hbm.at[span, :], sems.at[number]
            )
        )
    for copy in copies:
        copy.start()
    for copy in copies:
        copy.wait()


def fused_body(sizes, queries, keys_text, values_text, patch_rows, patch_owner, patch_place, value_head):
    dp_count, ctx_count, tp_count = sizes
    _, token_count, query_width = queries.shape
    kv_width = keys_text.shape[2]
    row_count = patch_rows.shape[2]
    heads = query_width // HD
    groups = kv_width // HD
    dma = pltpu.SemaphoreType.DMA
    vmem = pl.BlockSpec(memory_space=pltpu.VMEM)
    anywhere = pl.BlockSpec(memory_space=pl.ANY)
    others = max(tp_count - 1, 1)
    inputs = (
        patch_owner[0, 0].reshape(1, row_count),
        patch_place[0],
        patch_rows[0, 0],
        keys_text[0],
        values_text[0],
        value_head.reshape(heads, HD),
        queries[0],
    )
    shapes = (
        jax.ShapeDtypeStruct((token_count, query_width), jnp.bfloat16),
        jax.ShapeDtypeStruct((1, token_count), jnp.float32),
    )
    attention, value_out = pl.pallas_call(
        functools.partial(fused_kernel, sizes),
        out_shape=shapes,
        in_specs=[pl.BlockSpec(memory_space=pltpu.HBM)] * 7,
        out_specs=(anywhere, vmem),
        scratch_shapes=[
            pltpu.VMEM((token_count, query_width), jnp.bfloat16),
            pltpu.VMEM((token_count, query_width), jnp.bfloat16),
            pltpu.VMEM((ctx_count, groups, 2, token_count, HD), jnp.bfloat16),
            pltpu.VMEM((ctx_count * dp_count, row_count, 2, kv_width), jnp.bfloat16),
            pltpu.VMEM((ctx_count * dp_count, 2, 1, row_count), jnp.int32),
            pltpu.VMEM((groups, ctx_count * token_count, HD), jnp.bfloat16),
            pltpu.VMEM((groups, ctx_count * token_count, 2 * HD), jnp.bfloat16),
            pltpu.VMEM((heads, HD), jnp.bfloat16),
            pltpu.VMEM((heads, HD), jnp.float32),
            pltpu.VMEM((1, token_count), jnp.float32),
            pltpu.VMEM((others, 1, token_count), jnp.float32),
            dma,
            dma,
            dma((3,)),
            dma,
            dma((ctx_count, groups)),
            dma,
            dma((2,)),
            dma((ctx_count, 2)),
            dma((2,)),
            dma((others,)),
            dma((others,)),
            pltpu.SemaphoreType.REGULAR((dp_count + 1,)),
        ],
        compiler_params=pltpu.CompilerParams(
            collective_id=0, has_side_effects=True, vmem_limit_bytes=24 * 2**20
        ),
        name="merged_attention",
    )(*(pltpu.with_memory_space_constraint(array, pltpu.HBM) for array in inputs))
    attention, value_out = pl.pallas_call(
        write_kernel,
        out_shape=shapes,
        in_specs=[anywhere] * 2,
        out_specs=(pl.BlockSpec(memory_space=pltpu.HBM),) * 2,
        scratch_shapes=[dma((math.gcd(token_count // 16, 4) + 1,))],
        compiler_params=pltpu.CompilerParams(vmem_limit_bytes=2**20),
        name="write_out",
    )(*(pltpu.with_memory_space_constraint(array, pltpu.VMEM) for array in (attention, value_out)))
    return (attention[None], value_out)


def body(sizes, queries, keys_text, values_text, patch_rows, patch_owner, patch_place, value_head):
    dp_count, ctx_count, _ = sizes
    arriving = dp_count * ctx_count * patch_rows.size * patch_rows.dtype.itemsize
    arrays = (queries, keys_text, values_text, patch_rows, patch_owner, patch_place, value_head)
    if arriving > SLOT_BYTES or ctx_count % 2:
        return collective_body(*arrays)
    return fused_body(sizes, *arrays)


def solution(mesh):
    in_specs = (
        P("dp", "ctx", "tp"),
        P("dp", "ctx", "tp"),
        P("dp", "ctx", "tp"),
        P("dp", "ctx", None, None, "tp"),
        P("dp", "ctx", None, None),
        P("dp", "ctx", None),
        P("tp"),
    )
    out_specs = (P("dp", "ctx", "tp"), P("dp", "ctx"))
    sizes = tuple(mesh.shape[axis] for axis in ("dp", "ctx", "tp"))
    return jax.shard_map(
        functools.partial(body, sizes),
        mesh=mesh,
        in_specs=in_specs,
        out_specs=out_specs,
        check_vma=False,
    )
```

```python
import functools
import math

import jax
import jax.numpy as jnp
from jax import lax
from jax.experimental import pallas as pl
from jax.experimental.pallas import tpu as pltpu
from jax.sharding import PartitionSpec as P

HD = 128
CAP = 4
SLOT_BYTES = 8 * 2**20
MESH = pl.DeviceIdType.MESH


def attend_block(
    carried, query_split, query_place, block_keys, block_values, key_place, score_scale
):
    running_max, denominator, numerator = carried
    scores = (
        jnp.einsum("tgrd,sgd->tgrs", query_split, block_keys, preferred_element_type=jnp.float32)
        * score_scale
    )
    allowed = (key_place[None, :] <= query_place[:, None])[:, None, None, :]
    scores = jnp.where(allowed, scores, -1e30)
    new_max = jnp.maximum(running_max, jnp.max(scores, axis=-1))
    weights = jnp.where(allowed, jnp.exp(scores - new_max[..., None]), 0.0)
    shrink = jnp.exp(running_max - new_max)
    denominator = denominator * shrink + jnp.sum(weights, axis=-1)
    numerator = numerator * shrink[..., None] + jnp.einsum(
        "tgrs,sgd->tgrd",
        weights.astype(jnp.bfloat16),
        block_values,
        preferred_element_type=jnp.float32,
    )
    return (new_max, denominator, numerator)


def unchanged(carried):
    return carried


def collective_body(queries, keys_text, values_text, patch_rows, patch_owner, patch_place, value_head):
    token_count = queries.shape[1]
    kv_width = keys_text.shape[2]
    groups = kv_width // HD
    head_count = queries.shape[2] // HD
    group_size = head_count // groups
    score_scale = HD ** (-0.5)
    dp_count = lax.axis_size("dp")
    slot_count = dp_count * CAP
    owner_seq = patch_owner[0, 0, :, 0]
    places = patch_place[0, 0]
    owner_hits = (owner_seq[:, None] == jnp.arange(dp_count, dtype=jnp.int32)[None, :]).astype(
        jnp.int32
    )
    before = jnp.cumsum(owner_hits, axis=0) - owner_hits
    slot_rank = jnp.sum(before * owner_hits, axis=1)
    target = owner_seq * CAP + slot_rank
    select = (jnp.arange(slot_count, dtype=jnp.int32)[:, None] == target[None, :]).astype(jnp.int32)
    row_data = patch_rows[0, 0].reshape(places.shape[0], 2 * kv_width)
    packed = jnp.dot(
        select.astype(jnp.bfloat16), row_data, preferred_element_type=jnp.float32
    ).astype(jnp.bfloat16)
    filled = jnp.sum(select, axis=1)
    slot_place = jnp.sum(select * places[None, :], axis=1) + (1 - filled) * token_count
    packed = packed.reshape(slot_count, 2, kv_width)
    arrived, arrived_place = (
        lax.all_to_all(packed, "dp", split_axis=0, concat_axis=0, tiled=True),
        lax.all_to_all(slot_place, "dp", split_axis=0, concat_axis=0, tiled=True),
    )
    landing = (jnp.arange(token_count, dtype=jnp.int32)[:, None] == arrived_place[None, :]).astype(
        jnp.bfloat16
    )
    arrivals = jnp.dot(
        landing, arrived.reshape(slot_count, 2 * kv_width), preferred_element_type=jnp.float32
    )
    merged_keys = (keys_text[0].astype(jnp.float32) + arrivals[:, :kv_width]).astype(jnp.bfloat16)
    merged_values = (values_text[0].astype(jnp.float32) + arrivals[:, kv_width:]).astype(
        jnp.bfloat16
    )
    query_split = queries[0].reshape(token_count, groups, group_size, HD)
    first_row = lax.axis_index("ctx") * token_count
    query_place = first_row + jnp.arange(token_count, dtype=jnp.int32)
    initial = (
        jnp.full((token_count, groups, group_size), -1e30, jnp.float32),
        jnp.zeros((token_count, groups, group_size), jnp.float32),
        jnp.zeros((token_count, groups, group_size, HD), jnp.float32),
    )
    carried = initial
    start_row = jnp.int32(0)
    piece_keys = lax.all_gather(merged_keys, "ctx", axis=0, tiled=True)
    piece_values = lax.all_gather(merged_values, "ctx", axis=0, tiled=True)
    piece_rows = piece_keys.shape[0]
    block_rows = min(512, piece_rows)
    for lower in range(0, piece_rows, block_rows):
        upper = min(lower + block_rows, piece_rows)
        block_keys = piece_keys[lower:upper].reshape(upper - lower, groups, HD)
        block_values = piece_values[lower:upper].reshape(upper - lower, groups, HD)
        key_place = start_row + lower + jnp.arange(upper - lower, dtype=jnp.int32)

        def update(state_in):
            return attend_block(
                state_in, query_split, query_place, block_keys, block_values, key_place, score_scale
            )

        carried = lax.cond(
            start_row + lower <= first_row + token_count - 1, update, unchanged, carried
        )
    running_max, denominator, numerator = carried
    attention = (
        (numerator / denominator[..., None])
        .reshape(token_count, head_count * HD)
        .astype(jnp.bfloat16)
    )
    partial_value = jnp.dot(attention, value_head, preferred_element_type=jnp.float32)
    value_out = lax.psum(partial_value, "tp")
    return (attention[None], value_out[None])


def attend(queries, merged_keys, merged_values, probe, out, last, group, totals):
    token_count, width = queries.shape
    groups = merged_keys.shape[0]
    group_size = width // HD // groups
    length = (last + 1) * token_count
    rows = token_count // len(totals)
    score_scale = HD ** (-0.5) * math.log2(math.e)
    heads = range(group * group_size, (group + 1) * group_size)
    block_keys = merged_keys[group, 0:length, :]
    summed = len(totals) > 1
    block_values = merged_values[group, 0:length, 0 : 2 * HD if summed else HD]
    for number in range(len(totals)):
        lower = number * rows
        span = slice(lower, lower + rows)
        stacked = jnp.concatenate(
            [queries[span, head * HD : (head + 1) * HD] for head in heads], axis=0
        )
        scores = lax.dot_general(
            stacked, block_keys, (((1,), (1,)), ((), ())), preferred_element_type=jnp.float32
        )
        row = lower + lax.broadcasted_iota(jnp.int32, (rows, token_count), 0)
        col = lax.broadcasted_iota(jnp.int32, (rows, token_count), 1)
        allowed = jnp.concatenate([col <= row] * group_size, axis=0)
        parts = [scores[:, j * token_count : (j + 1) * token_count] for j in range(last + 1)]
        parts[last] = jnp.where(allowed, parts[last], -1e30)
        top = jnp.max(functools.reduce(jnp.maximum, parts), axis=1, keepdims=True)
        weights = [jnp.exp2((part - top) * score_scale) for part in parts]
        rounded = jnp.concatenate([w.astype(jnp.bfloat16) for w in weights], axis=1)
        sums = jnp.dot(rounded, block_values, preferred_element_type=jnp.float32)
        if summed:
            denominator = sums[:, HD:]
        else:
            denominator = jnp.sum(functools.reduce(jnp.add, weights), axis=1, keepdims=True)
        result = (sums[:, :HD] * (1.0 / denominator)).astype(jnp.bfloat16)
        for extra, head in enumerate(heads):
            piece = result[extra * rows : (extra + 1) * rows]
            out[span, head * HD : (head + 1) * HD] = piece
            totals[number] = (
                totals[number] + piece.astype(jnp.float32) * probe[head : head + 1, :]
            )


def fused_kernel(
    sizes,
    owner_hbm,
    place_hbm,
    rows_hbm,
    keys_hbm,
    values_hbm,
    probe_hbm,
    queries_hbm,
    out_any,
    value_ref,
    queries,
    out,
    text,
    rows_in,
    spots_in,
    merged_keys,
    merged_values,
    probe_raw,
    probe,
    partial,
    partial_in,
    query_sem,
    out_sem,
    local_sem,
    text_send,
    text_recv,
    relay_send,
    patch_send,
    patch_recv,
    pass_send,
    value_send,
    value_recv,
    ready,
):
    dp_count, ctx_count, tp_count = sizes
    d, c, t = lax.axis_index("dp"), lax.axis_index("ctx"), lax.axis_index("tp")
    token_count, kv_width = keys_hbm.shape
    row_count = rows_hbm.shape[0]
    groups = kv_width // HD
    heads = queries.shape[1] // HD
    chips = ctx_count // 2
    side = lax.rem(c, 2)
    chip = c // 2
    partner = c + 1 - 2 * side

    barrier = pltpu.get_barrier_semaphore()
    in_pair = dp_count

    def greet(*device):
        pl.semaphore_signal(barrier, inc=1, device_id=device, device_id_type=MESH)

    def over(lower, upper, act):
        def step(number, carry):
            act(number)
            return carry

        lax.fori_loop(lower, upper, step, 0)

    over(1, ctx_count, lambda step: greet(d, lax.rem(c + step, ctx_count), t))
    over(t + 1, tp_count, lambda other: greet(d, c, other))

    def greet_plane(there):
        for block in range(ctx_count):
            greet(there, block, t)

    over(d + 1, dp_count, greet_plane)

    def lanes(group):
        return slice(group * HD, (group + 1) * HD)

    def copy_of(src, dst, sem):
        return pltpu.make_async_copy(src, dst, sem)

    def wait_bytes(ref, sem):
        copy_of(ref, ref, sem).wait()

    own = c * dp_count + d
    load_patches = [
        copy_of(rows_hbm, rows_in.at[own], local_sem.at[0]),
        copy_of(owner_hbm, spots_in.at[own, 0], local_sem.at[1]),
        copy_of(place_hbm, spots_in.at[own, 1], local_sem.at[1]),
    ]
    load_probe = copy_of(probe_hbm, probe_raw, local_sem.at[2])
    load_queries = copy_of(queries_hbm, queries, query_sem)
    for load in load_patches:
        load.start()
    for group in range(groups):
        for kind, source in enumerate((keys_hbm, values_hbm)):
            copy_of(
                source.at[:, lanes(group)], text.at[c, group, kind], text_recv.at[c, group]
            ).start()
    load_probe.start()
    load_queries.start()
    merged_values[:, :, HD:] = jnp.ones((groups, ctx_count * token_count, HD), jnp.bfloat16)
    with jax.named_scope("w_barrier"):
        pl.semaphore_wait(barrier, d * ctx_count + ctx_count - 1 + t)

    def announce(number, *device):
        pl.semaphore_signal(
            ready.at[number], inc=1, device_id=device, device_id_type=MESH
        )

    over(
        0,
        d,
        lambda there: over(c * (1 - side), c + 1, lambda block: announce(d, there, block, t)),
    )
    over(0, t, lambda other: announce(in_pair, d, c, other))
    with jax.named_scope("w_loads"):
        wait_bytes(rows_in.at[own], local_sem.at[0])
        wait_bytes(spots_in.at[own], local_sem.at[1])

    parts = (rows_in, spots_in)
    targets = chips - chip - side

    def send_patches(there, own_block):
        def to_block(block):
            for kind, part in enumerate(parts):
                pltpu.make_async_remote_copy(
                    src_ref=part.at[own],
                    dst_ref=part.at[own],
                    send_sem=patch_send.at[kind],
                    recv_sem=patch_recv.at[c, kind],
                    device_id=(there, block, t),
                    device_id_type=MESH,
                ).start()

        if own_block:
            to_block(c)
        over(chip + side, chips, lambda m: to_block(2 * m + 1))

    with jax.named_scope("down"):
        over(0, d, lambda there: send_patches(there, True))
    send_patches(d, False)
    with jax.named_scope("w_text"):
        for group in range(groups):
            wait_bytes(text.at[c, group], text_recv.at[c, group])

    def text_copy(group, block, there, sem):
        return pltpu.make_async_remote_copy(
            src_ref=text.at[block, group],
            dst_ref=text.at[block, group],
            send_sem=sem,
            recv_sem=text_recv.at[block, group],
            device_id=(d, there, t),
            device_id_type=MESH,
        )

    with jax.named_scope("texts"):
        for group in range(groups):
            hub = (group + 1) % 2
            over(
                chip + 1, chips, lambda m: text_copy(group, c, 2 * m + hub, text_send).start()
            )

            @pl.when(side == 0)
            def _():
                text_copy(group, c, c + 1, text_send).start()

    load_probe.wait()
    probe[...] = probe_raw[...].astype(jnp.float32)

    def send_up(there):
        pl.semaphore_wait(ready.at[there], targets + 1)
        send_patches(there, True)

    def relay(group):
        def hand_on(block):
            wait_bytes(text.at[block, group], text_recv.at[block, group])
            text_copy(group, block, partner, relay_send.at[group]).start()

        @pl.when(side == (group + 1) % 2)
        def _():
            over(0, 2 * chip, hand_on)

    with jax.named_scope("up"):
        over(d + 1, dp_count, send_up)
    with jax.named_scope("relay"):
        for group in range(groups):
            relay(group)

    def pass_patches(block):
        span = pl.ds(block * dp_count, dp_count)
        for kind, part in enumerate(parts):
            pltpu.make_async_remote_copy(
                src_ref=part.at[span],
                dst_ref=part.at[span],
                send_sem=pass_send.at[kind],
                recv_sem=patch_recv.at[block, kind],
                device_id=(d, c - 1, t),
                device_id_type=MESH,
            ).start()

    def merge(block, chosen):
        slots = dp_count * row_count
        span = slice(block * dp_count, (block + 1) * dp_count)
        spots = spots_in[span]
        code = spots[:, 0] * token_count + spots[:, 1]
        code = jnp.concatenate([code[k] for k in range(dp_count)], axis=1)
        here = d * token_count + lax.broadcasted_iota(jnp.int32, (token_count, slots), 0)
        landing = jnp.where(code == here, 1.0, 0.0).astype(jnp.bfloat16)
        wide = slice(chosen[0] * HD, (chosen[-1] + 1) * HD)
        rows = rows_in[span, :, :, wide].astype(jnp.float32)
        tokens = slice(block * token_count, (block + 1) * token_count)
        for kind in range(2):
            kind_rows = rows[:, :, kind, :].reshape(slots, -1).astype(jnp.bfloat16)
            arrivals = jnp.dot(landing, kind_rows, preferred_element_type=jnp.float32)
            for number, group in enumerate(chosen):
                whole = text[block, group, kind].astype(jnp.float32) + arrivals[:, lanes(number)]
                if kind == 0:
                    merged_keys[group, tokens, :] = whole.astype(jnp.bfloat16)
                else:
                    merged_values[group, tokens, 0:HD] = whole.astype(jnp.bfloat16)

    def finish(last):
        with jax.named_scope("w_patch"):
            for block in range(last + 1):
                senders = dp_count if block < last else dp_count - 1
                for kind, part in enumerate(parts):
                    wait_bytes(
                        part.at[pl.ds(block * dp_count, senders)], patch_recv.at[block, kind]
                    )
                if last % 2 and block < last - 1:
                    pass_patches(block)
        with jax.named_scope("w_kv"):
            for group in range(groups):
                relayed = 0 if last % 2 != (group + 1) % 2 else 2 * (last // 2)
                for block in range(relayed, last):
                    wait_bytes(text.at[block, group], text_recv.at[block, group])
            load_queries.wait()
        with jax.named_scope("attend"):
            rows = math.gcd(token_count, 16) if last % 2 and last > 1 else token_count
            totals = [jnp.zeros((rows, HD), jnp.float32)] * (token_count // rows)
            for block in range(last + 1):
                merge(block, range(groups))
            for group in range(groups):
                attend(queries, merged_keys, merged_values, probe, out, last, group, totals)
        total = jnp.concatenate(totals, axis=0)
        partial[...] = jnp.sum(jnp.transpose(total), axis=0, keepdims=True)

    for last in range(ctx_count):

        @pl.when(c == last)
        def _():
            finish(last)

    value_copies = [
        pltpu.make_async_remote_copy(
            src_ref=partial,
            dst_ref=partial_in.at[k - 1],
            send_sem=value_send.at[k - 1],
            recv_sem=value_recv.at[k - 1],
            device_id=(d, c, lax.rem(t + k, tp_count)),
            device_id_type=MESH,
        )
        for k in range(1, tp_count)
    ]
    with jax.named_scope("w_pair"):

        @pl.when(t < tp_count - 1)
        def _():
            pl.semaphore_wait(ready.at[in_pair], tp_count - 1 - t)

    for copy in value_copies:
        copy.start()
    store = copy_of(out, out_any, out_sem)
    store.start()
    with jax.named_scope("tail"):
        for last in range(ctx_count):

            @pl.when(c == last)
            def _():
                sent = dp_count * (chips - last // 2 - last % 2 + 1) - 1
                for kind, part in enumerate(parts):
                    if sent:
                        wait_bytes(part.at[pl.ds(0, sent)], patch_send.at[kind])
                    if last % 2 and last > 1:
                        wait_bytes(part.at[pl.ds(0, (last - 1) * dp_count)], pass_send.at[kind])
                copies = chips - last // 2 - last % 2
                if copies:
                    wait_bytes(text.at[pl.ds(0, copies)], text_send)
                for group in range(groups):
                    if last > 1 and last % 2 == (group + 1) % 2:
                        wait_bytes(text.at[pl.ds(0, 2 * (last // 2)), group], relay_send.at[group])

        store.wait()
        for copy in value_copies:
            copy.wait()
    whole = partial[...]
    for k in range(1, tp_count):
        whole = whole + partial_in[k - 1]
    value_ref[...] = whole


def write_kernel(attention, value, attention_hbm, value_hbm, sems):
    pieces = sems.shape[0] - 1
    rows = attention.shape[0] // pieces
    copies = [pltpu.make_async_copy(value, value_hbm, sems.at[pieces])]
    for number in range(pieces):
        span = pl.ds(number * rows, rows)
        copies.append(
            pltpu.make_async_copy(
                attention.at[span, :], attention_hbm.at[span, :], sems.at[number]
            )
        )
    for copy in copies:
        copy.start()
    for copy in copies:
        copy.wait()


def fused_body(sizes, queries, keys_text, values_text, patch_rows, patch_owner, patch_place, value_head):
    dp_count, ctx_count, tp_count = sizes
    _, token_count, query_width = queries.shape
    kv_width = keys_text.shape[2]
    row_count = patch_rows.shape[2]
    heads = query_width // HD
    groups = kv_width // HD
    dma = pltpu.SemaphoreType.DMA
    vmem = pl.BlockSpec(memory_space=pltpu.VMEM)
    anywhere = pl.BlockSpec(memory_space=pl.ANY)
    others = max(tp_count - 1, 1)
    inputs = (
        patch_owner[0, 0].reshape(1, row_count),
        patch_place[0],
        patch_rows[0, 0],
        keys_text[0],
        values_text[0],
        value_head.reshape(heads, HD),
        queries[0],
    )
    shapes = (
        jax.ShapeDtypeStruct((token_count, query_width), jnp.bfloat16),
        jax.ShapeDtypeStruct((1, token_count), jnp.float32),
    )
    attention, value_out = pl.pallas_call(
        functools.partial(fused_kernel, sizes),
        out_shape=shapes,
        in_specs=[pl.BlockSpec(memory_space=pltpu.HBM)] * 7,
        out_specs=(anywhere, vmem),
        scratch_shapes=[
            pltpu.VMEM((token_count, query_width), jnp.bfloat16),
            pltpu.VMEM((token_count, query_width), jnp.bfloat16),
            pltpu.VMEM((ctx_count, groups, 2, token_count, HD), jnp.bfloat16),
            pltpu.VMEM((ctx_count * dp_count, row_count, 2, kv_width), jnp.bfloat16),
            pltpu.VMEM((ctx_count * dp_count, 2, 1, row_count), jnp.int32),
            pltpu.VMEM((groups, ctx_count * token_count, HD), jnp.bfloat16),
            pltpu.VMEM((groups, ctx_count * token_count, 2 * HD), jnp.bfloat16),
            pltpu.VMEM((heads, HD), jnp.bfloat16),
            pltpu.VMEM((heads, HD), jnp.float32),
            pltpu.VMEM((1, token_count), jnp.float32),
            pltpu.VMEM((others, 1, token_count), jnp.float32),
            dma,
            dma,
            dma((3,)),
            dma,
            dma((ctx_count, groups)),
            dma((groups,)),
            dma((2,)),
            dma((ctx_count, 2)),
            dma((2,)),
            dma((others,)),
            dma((others,)),
            pltpu.SemaphoreType.REGULAR((dp_count + 1,)),
        ],
        compiler_params=pltpu.CompilerParams(
            collective_id=0, has_side_effects=True, vmem_limit_bytes=24 * 2**20
        ),
        name="merged_attention",
    )(*(pltpu.with_memory_space_constraint(array, pltpu.HBM) for array in inputs))
    attention, value_out = pl.pallas_call(
        write_kernel,
        out_shape=shapes,
        in_specs=[anywhere] * 2,
        out_specs=(pl.BlockSpec(memory_space=pltpu.HBM),) * 2,
        scratch_shapes=[dma((math.gcd(token_count // 16, 4) + 1,))],
        compiler_params=pltpu.CompilerParams(vmem_limit_bytes=2**20),
        name="write_out",
    )(*(pltpu.with_memory_space_constraint(array, pltpu.VMEM) for array in (attention, value_out)))
    return (attention[None], value_out)


def body(sizes, queries, keys_text, values_text, patch_rows, patch_owner, patch_place, value_head):
    dp_count, ctx_count, _ = sizes
    arriving = dp_count * ctx_count * patch_rows.size * patch_rows.dtype.itemsize
    arrays = (queries, keys_text, values_text, patch_rows, patch_owner, patch_place, value_head)
    if arriving > SLOT_BYTES or ctx_count % 2:
        return collective_body(*arrays)
    return fused_body(sizes, *arrays)


def solution(mesh):
    in_specs = (
        P("dp", "ctx", "tp"),
        P("dp", "ctx", "tp"),
        P("dp", "ctx", "tp"),
        P("dp", "ctx", None, None, "tp"),
        P("dp", "ctx", None, None),
        P("dp", "ctx", None),
        P("tp"),
    )
    out_specs = (P("dp", "ctx", "tp"), P("dp", "ctx"))
    sizes = tuple(mesh.shape[axis] for axis in ("dp", "ctx", "tp"))
    return jax.shard_map(
        functools.partial(body, sizes),
        mesh=mesh,
        in_specs=in_specs,
        out_specs=out_specs,
        check_vma=False,
    )
```

```python
import functools
import math

import jax
import jax.numpy as jnp
from jax import lax
from jax.experimental import pallas as pl
from jax.experimental.pallas import tpu as pltpu
from jax.sharding import PartitionSpec as P

HD = 128
CAP = 4
SLOT_BYTES = 8 * 2**20
MESH = pl.DeviceIdType.MESH


def attend_block(
    carried, query_split, query_place, block_keys, block_values, key_place, score_scale
):
    running_max, denominator, numerator = carried
    scores = (
        jnp.einsum("tgrd,sgd->tgrs", query_split, block_keys, preferred_element_type=jnp.float32)
        * score_scale
    )
    allowed = (key_place[None, :] <= query_place[:, None])[:, None, None, :]
    scores = jnp.where(allowed, scores, -1e30)
    new_max = jnp.maximum(running_max, jnp.max(scores, axis=-1))
    weights = jnp.where(allowed, jnp.exp(scores - new_max[..., None]), 0.0)
    shrink = jnp.exp(running_max - new_max)
    denominator = denominator * shrink + jnp.sum(weights, axis=-1)
    numerator = numerator * shrink[..., None] + jnp.einsum(
        "tgrs,sgd->tgrd",
        weights.astype(jnp.bfloat16),
        block_values,
        preferred_element_type=jnp.float32,
    )
    return (new_max, denominator, numerator)


def unchanged(carried):
    return carried


def collective_body(queries, keys_text, values_text, patch_rows, patch_owner, patch_place, value_head):
    token_count = queries.shape[1]
    kv_width = keys_text.shape[2]
    groups = kv_width // HD
    head_count = queries.shape[2] // HD
    group_size = head_count // groups
    score_scale = HD ** (-0.5)
    dp_count = lax.axis_size("dp")
    slot_count = dp_count * CAP
    owner_seq = patch_owner[0, 0, :, 0]
    places = patch_place[0, 0]
    owner_hits = (owner_seq[:, None] == jnp.arange(dp_count, dtype=jnp.int32)[None, :]).astype(
        jnp.int32
    )
    before = jnp.cumsum(owner_hits, axis=0) - owner_hits
    slot_rank = jnp.sum(before * owner_hits, axis=1)
    target = owner_seq * CAP + slot_rank
    select = (jnp.arange(slot_count, dtype=jnp.int32)[:, None] == target[None, :]).astype(jnp.int32)
    row_data = patch_rows[0, 0].reshape(places.shape[0], 2 * kv_width)
    packed = jnp.dot(
        select.astype(jnp.bfloat16), row_data, preferred_element_type=jnp.float32
    ).astype(jnp.bfloat16)
    filled = jnp.sum(select, axis=1)
    slot_place = jnp.sum(select * places[None, :], axis=1) + (1 - filled) * token_count
    packed = packed.reshape(slot_count, 2, kv_width)
    arrived, arrived_place = (
        lax.all_to_all(packed, "dp", split_axis=0, concat_axis=0, tiled=True),
        lax.all_to_all(slot_place, "dp", split_axis=0, concat_axis=0, tiled=True),
    )
    landing = (jnp.arange(token_count, dtype=jnp.int32)[:, None] == arrived_place[None, :]).astype(
        jnp.bfloat16
    )
    arrivals = jnp.dot(
        landing, arrived.reshape(slot_count, 2 * kv_width), preferred_element_type=jnp.float32
    )
    merged_keys = (keys_text[0].astype(jnp.float32) + arrivals[:, :kv_width]).astype(jnp.bfloat16)
    merged_values = (values_text[0].astype(jnp.float32) + arrivals[:, kv_width:]).astype(
        jnp.bfloat16
    )
    query_split = queries[0].reshape(token_count, groups, group_size, HD)
    first_row = lax.axis_index("ctx") * token_count
    query_place = first_row + jnp.arange(token_count, dtype=jnp.int32)
    initial = (
        jnp.full((token_count, groups, group_size), -1e30, jnp.float32),
        jnp.zeros((token_count, groups, group_size), jnp.float32),
        jnp.zeros((token_count, groups, group_size, HD), jnp.float32),
    )
    carried = initial
    start_row = jnp.int32(0)
    piece_keys = lax.all_gather(merged_keys, "ctx", axis=0, tiled=True)
    piece_values = lax.all_gather(merged_values, "ctx", axis=0, tiled=True)
    piece_rows = piece_keys.shape[0]
    block_rows = min(512, piece_rows)
    for lower in range(0, piece_rows, block_rows):
        upper = min(lower + block_rows, piece_rows)
        block_keys = piece_keys[lower:upper].reshape(upper - lower, groups, HD)
        block_values = piece_values[lower:upper].reshape(upper - lower, groups, HD)
        key_place = start_row + lower + jnp.arange(upper - lower, dtype=jnp.int32)

        def update(state_in):
            return attend_block(
                state_in, query_split, query_place, block_keys, block_values, key_place, score_scale
            )

        carried = lax.cond(
            start_row + lower <= first_row + token_count - 1, update, unchanged, carried
        )
    running_max, denominator, numerator = carried
    attention = (
        (numerator / denominator[..., None])
        .reshape(token_count, head_count * HD)
        .astype(jnp.bfloat16)
    )
    partial_value = jnp.dot(attention, value_head, preferred_element_type=jnp.float32)
    value_out = lax.psum(partial_value, "tp")
    return (attention[None], value_out[None])


def attend(queries, merged_keys, merged_values, probe, out, last, group, totals):
    token_count, width = queries.shape
    groups = merged_keys.shape[0]
    group_size = width // HD // groups
    length = (last + 1) * token_count
    rows = token_count // len(totals)
    score_scale = HD ** (-0.5) * math.log2(math.e)
    heads = range(group * group_size, (group + 1) * group_size)
    block_keys = merged_keys[group, 0:length, :]
    summed = len(totals) > 1
    block_values = merged_values[group, 0:length, 0 : 2 * HD if summed else HD]
    for number in range(len(totals)):
        lower = number * rows
        span = slice(lower, lower + rows)
        stacked = jnp.concatenate(
            [queries[span, head * HD : (head + 1) * HD] for head in heads], axis=0
        )
        scores = lax.dot_general(
            stacked, block_keys, (((1,), (1,)), ((), ())), preferred_element_type=jnp.float32
        )
        row = lower + lax.broadcasted_iota(jnp.int32, (rows, token_count), 0)
        col = lax.broadcasted_iota(jnp.int32, (rows, token_count), 1)
        allowed = jnp.concatenate([col <= row] * group_size, axis=0)
        parts = [scores[:, j * token_count : (j + 1) * token_count] for j in range(last + 1)]
        parts[last] = jnp.where(allowed, parts[last], -1e30)
        top = jnp.max(functools.reduce(jnp.maximum, parts), axis=1, keepdims=True)
        weights = [jnp.exp2((part - top) * score_scale) for part in parts]
        rounded = jnp.concatenate([w.astype(jnp.bfloat16) for w in weights], axis=1)
        sums = jnp.dot(rounded, block_values, preferred_element_type=jnp.float32)
        if summed:
            denominator = sums[:, HD:]
        else:
            denominator = jnp.sum(functools.reduce(jnp.add, weights), axis=1, keepdims=True)
        result = (sums[:, :HD] * (1.0 / denominator)).astype(jnp.bfloat16)
        for extra, head in enumerate(heads):
            piece = result[extra * rows : (extra + 1) * rows]
            out[span, head * HD : (head + 1) * HD] = piece
            totals[number] = (
                totals[number] + piece.astype(jnp.float32) * probe[head : head + 1, :]
            )


def fused_kernel(
    sizes,
    owner_hbm,
    place_hbm,
    rows_hbm,
    keys_hbm,
    values_hbm,
    probe_hbm,
    queries_hbm,
    out_any,
    value_ref,
    queries,
    out,
    text,
    rows_in,
    spots_in,
    merged_keys,
    merged_values,
    probe_raw,
    probe,
    partial,
    partial_in,
    query_sem,
    out_sem,
    local_sem,
    text_recv,
    patch_recv,
    pass_send,
    value_recv,
    ready,
):
    dp_count, ctx_count, tp_count = sizes
    d, c, t = lax.axis_index("dp"), lax.axis_index("ctx"), lax.axis_index("tp")
    token_count, kv_width = keys_hbm.shape
    row_count = rows_hbm.shape[0]
    groups = kv_width // HD
    heads = queries.shape[1] // HD
    chips = ctx_count // 2
    side = lax.rem(c, 2)
    chip = c // 2
    partner = c + 1 - 2 * side

    barrier = pltpu.get_barrier_semaphore()
    in_pair = dp_count - 1

    def greet(*device):
        pl.semaphore_signal(barrier, inc=1, device_id=device, device_id_type=MESH)

    def over(lower, upper, act):
        def step(number, carry):
            act(number)
            return carry

        lax.fori_loop(lower, upper, step, 0)

    over(1, ctx_count, lambda step: greet(d, lax.rem(c + step, ctx_count), t))
    over(t + 1, tp_count, lambda other: greet(d, c, other))

    def greet_plane(there):
        for block in range(ctx_count):
            greet(there, block, t)

    over(d + 1, dp_count, greet_plane)

    def lanes(group):
        return slice(group * HD, (group + 1) * HD)

    def copy_of(src, dst, sem):
        return pltpu.make_async_copy(src, dst, sem)

    def wait_bytes(ref, sem):
        copy_of(ref, ref, sem).wait()

    patch_send, text_send, relay_send, value_send = local_sem, local_sem.at[2], local_sem.at[3], query_sem
    own = c * dp_count + d
    load_patches = [
        copy_of(rows_hbm, rows_in.at[own], local_sem.at[0]),
        copy_of(owner_hbm, spots_in.at[own, 0], local_sem.at[1]),
        copy_of(place_hbm, spots_in.at[own, 1], local_sem.at[1]),
    ]
    load_probe = copy_of(probe_hbm, probe_raw, local_sem.at[2])
    load_queries = copy_of(queries_hbm, queries, query_sem.at[0])
    for load in load_patches:
        load.start()
    for group in range(groups):
        for kind, source in enumerate((keys_hbm, values_hbm)):
            copy_of(
                source.at[:, lanes(group)], text.at[c, group, kind], local_sem.at[3]
            ).start()
    load_probe.start()
    load_queries.start()
    merged_values[:, :, HD:] = jnp.ones((groups, ctx_count * token_count, HD), jnp.bfloat16)
    with jax.named_scope("w_barrier"):
        pl.semaphore_wait(barrier, d * ctx_count + ctx_count - 1 + t)

    def announce(number, *device):
        pl.semaphore_signal(
            ready.at[number], inc=1, device_id=device, device_id_type=MESH
        )

    over(
        0,
        d,
        lambda there: over(c * (1 - side), c + 1, lambda block: announce(d - 1, there, block, t)),
    )
    over(0, t, lambda other: announce(in_pair, d, c, other))
    with jax.named_scope("w_loads"):
        wait_bytes(rows_in.at[own], local_sem.at[0])
        wait_bytes(spots_in.at[own], local_sem.at[1])

    parts = (rows_in, spots_in)
    targets = chips - chip - side

    def send_patches(there, own_block):
        def to_block(block):
            for kind, part in enumerate(parts):
                pltpu.make_async_remote_copy(
                    src_ref=part.at[own],
                    dst_ref=part.at[own],
                    send_sem=patch_send.at[kind],
                    recv_sem=patch_recv.at[kind],
                    device_id=(there, block, t),
                    device_id_type=MESH,
                ).start()

        if own_block:
            to_block(c)
        over(chip + side, chips, lambda m: to_block(2 * m + 1))

    with jax.named_scope("down"):
        over(0, d, lambda there: send_patches(there, True))
    send_patches(d, False)
    with jax.named_scope("w_text"):
        wait_bytes(text.at[c], local_sem.at[3])
        load_probe.wait()
        probe[...] = probe_raw[...].astype(jnp.float32)

    def text_copy(group, block, there, sem):
        return pltpu.make_async_remote_copy(
            src_ref=text.at[block, group],
            dst_ref=text.at[block, group],
            send_sem=sem,
            recv_sem=text_recv.at[group],
            device_id=(d, there, t),
            device_id_type=MESH,
        )

    with jax.named_scope("texts"):
        for group in range(groups):
            hub = (group + 1) % 2
            over(
                chip + 1, chips, lambda m: text_copy(group, c, 2 * m + hub, text_send).start()
            )

            @pl.when(side == 0)
            def _():
                text_copy(group, c, c + 1, text_send).start()

    def send_up(there):
        pl.semaphore_wait(ready.at[there - 1], targets + 1)
        send_patches(there, True)

    def relay(last, group):
        if last:
            wait_bytes(text.at[pl.ds(0, last), group], text_recv.at[group])
        if last % 2 == (group + 1) % 2:
            for block in range(2 * (last // 2)):
                text_copy(group, block, partner, relay_send).start()

    with jax.named_scope("up"):
        over(d + 1, dp_count, send_up)
    def pass_patches(block):
        span = pl.ds(block * dp_count, dp_count)
        for kind, part in enumerate(parts):
            pltpu.make_async_remote_copy(
                src_ref=part.at[span],
                dst_ref=part.at[span],
                send_sem=pass_send.at[kind],
                recv_sem=patch_recv.at[kind],
                device_id=(d, c - 1, t),
                device_id_type=MESH,
            ).start()

    def merge(block, chosen):
        slots = dp_count * row_count
        span = slice(block * dp_count, (block + 1) * dp_count)
        spots = spots_in[span]
        code = spots[:, 0] * token_count + spots[:, 1]
        code = jnp.concatenate([code[k] for k in range(dp_count)], axis=1)
        here = d * token_count + lax.broadcasted_iota(jnp.int32, (token_count, slots), 0)
        landing = jnp.where(code == here, 1.0, 0.0).astype(jnp.bfloat16)
        wide = slice(chosen[0] * HD, (chosen[-1] + 1) * HD)
        rows = rows_in[span, :, :, wide].astype(jnp.float32)
        tokens = slice(block * token_count, (block + 1) * token_count)
        for kind in range(2):
            kind_rows = rows[:, :, kind, :].reshape(slots, -1).astype(jnp.bfloat16)
            arrivals = jnp.dot(landing, kind_rows, preferred_element_type=jnp.float32)
            for number, group in enumerate(chosen):
                whole = text[block, group, kind].astype(jnp.float32) + arrivals[:, lanes(number)]
                if kind == 0:
                    merged_keys[group, tokens, :] = whole.astype(jnp.bfloat16)
                else:
                    merged_values[group, tokens, 0:HD] = whole.astype(jnp.bfloat16)

    def finish(last):
        hubs = [group for group in range(groups) if last % 2 == (group + 1) % 2]
        others = [group for group in range(groups) if group not in hubs]
        with jax.named_scope("relay"):
            for group in hubs:
                relay(last, group)
        with jax.named_scope("w_patch"):
            for kind, part in enumerate(parts):
                wait_bytes(part.at[pl.ds(0, (last + 1) * dp_count - 1)], patch_recv.at[kind])
            if last % 2:
                for block in range(last - 1):
                    pass_patches(block)
        with jax.named_scope("w_kv"):
            for group in others:
                relay(last, group)
            load_queries.wait()
        with jax.named_scope("attend"):
            rows = math.gcd(token_count, 16) if last % 2 and last > 1 else token_count
            totals = [jnp.zeros((rows, HD), jnp.float32)] * (token_count // rows)
            for block in range(last + 1):
                merge(block, range(groups))
            for group in range(groups):
                attend(queries, merged_keys, merged_values, probe, out, last, group, totals)
        total = jnp.concatenate(totals, axis=0)
        partial[...] = jnp.sum(jnp.transpose(total), axis=0, keepdims=True)

    for last in range(ctx_count):

        @pl.when(c == last)
        def _():
            finish(last)

    value_copies = [
        pltpu.make_async_remote_copy(
            src_ref=partial,
            dst_ref=partial_in.at[k - 1],
            send_sem=value_send.at[k - 1],
            recv_sem=value_recv.at[k - 1],
            device_id=(d, c, lax.rem(t + k, tp_count)),
            device_id_type=MESH,
        )
        for k in range(1, tp_count)
    ]
    with jax.named_scope("w_pair"):

        @pl.when(t < tp_count - 1)
        def _():
            pl.semaphore_wait(ready.at[in_pair], tp_count - 1 - t)

    for copy in value_copies:
        copy.start()
    store = copy_of(out, out_any, out_sem)
    store.start()
    with jax.named_scope("tail"):
        for last in range(ctx_count):

            @pl.when(c == last)
            def _():
                sent = dp_count * (chips - last // 2 - last % 2 + 1) - 1
                for kind, part in enumerate(parts):
                    if sent:
                        wait_bytes(part.at[pl.ds(0, sent)], patch_send.at[kind])
                    if last % 2 and last > 1:
                        wait_bytes(part.at[pl.ds(0, (last - 1) * dp_count)], pass_send.at[kind])
                copies = chips - last // 2 - last % 2
                if copies:
                    wait_bytes(text.at[pl.ds(0, copies)], text_send)
                relayed = 2 * (last // 2) * len([h for h in range(groups) if last % 2 == (h + 1) % 2])
                if relayed:
                    wait_bytes(text.at[pl.ds(0, relayed // groups)], relay_send)

        store.wait()
        for copy in value_copies:
            copy.wait()
    whole = partial[...]
    for k in range(1, tp_count):
        whole = whole + partial_in[k - 1]
    value_ref[...] = whole


def write_kernel(attention, value, attention_hbm, value_hbm, sems):
    pieces = sems.shape[0] - 1
    rows = attention.shape[0] // pieces
    copies = [pltpu.make_async_copy(value, value_hbm, sems.at[pieces])]
    for number in range(pieces):
        span = pl.ds(number * rows, rows)
        copies.append(
            pltpu.make_async_copy(
                attention.at[span, :], attention_hbm.at[span, :], sems.at[number]
            )
        )
    for copy in copies:
        copy.start()
    for copy in copies:
        copy.wait()


def fused_body(sizes, queries, keys_text, values_text, patch_rows, patch_owner, patch_place, value_head):
    dp_count, ctx_count, tp_count = sizes
    _, token_count, query_width = queries.shape
    kv_width = keys_text.shape[2]
    row_count = patch_rows.shape[2]
    heads = query_width // HD
    groups = kv_width // HD
    dma = pltpu.SemaphoreType.DMA
    vmem = pl.BlockSpec(memory_space=pltpu.VMEM)
    anywhere = pl.BlockSpec(memory_space=pl.ANY)
    others = max(tp_count - 1, 1)
    inputs = (
        patch_owner[0, 0].reshape(1, row_count),
        patch_place[0],
        patch_rows[0, 0],
        keys_text[0],
        values_text[0],
        value_head.reshape(heads, HD),
        queries[0],
    )
    shapes = (
        jax.ShapeDtypeStruct((token_count, query_width), jnp.bfloat16),
        jax.ShapeDtypeStruct((1, token_count), jnp.float32),
    )
    attention, value_out = pl.pallas_call(
        functools.partial(fused_kernel, sizes),
        out_shape=shapes,
        in_specs=[pl.BlockSpec(memory_space=pltpu.HBM)] * 7,
        out_specs=(anywhere, vmem),
        scratch_shapes=[
            pltpu.VMEM((token_count, query_width), jnp.bfloat16),
            pltpu.VMEM((token_count, query_width), jnp.bfloat16),
            pltpu.VMEM((ctx_count, groups, 2, token_count, HD), jnp.bfloat16),
            pltpu.VMEM((ctx_count * dp_count, row_count, 2, kv_width), jnp.bfloat16),
            pltpu.VMEM((ctx_count * dp_count, 2, 1, row_count), jnp.int32),
            pltpu.VMEM((groups, ctx_count * token_count, HD), jnp.bfloat16),
            pltpu.VMEM((groups, ctx_count * token_count, 2 * HD), jnp.bfloat16),
            pltpu.VMEM((heads, HD), jnp.bfloat16),
            pltpu.VMEM((heads, HD), jnp.float32),
            pltpu.VMEM((1, token_count), jnp.float32),
            pltpu.VMEM((others, 1, token_count), jnp.float32),
            dma((others,)),
            dma,
            dma((4,)),
            dma((groups,)),
            dma((2,)),
            dma((2,)),
            dma((others,)),
            pltpu.SemaphoreType.REGULAR((dp_count,)),
        ],
        compiler_params=pltpu.CompilerParams(
            collective_id=0, has_side_effects=True, vmem_limit_bytes=24 * 2**20
        ),
        name="merged_attention",
    )(*(pltpu.with_memory_space_constraint(array, pltpu.HBM) for array in inputs))
    attention, value_out = pl.pallas_call(
        write_kernel,
        out_shape=shapes,
        in_specs=[anywhere] * 2,
        out_specs=(pl.BlockSpec(memory_space=pltpu.HBM),) * 2,
        scratch_shapes=[dma((math.gcd(token_count // 16, 4) + 1,))],
        compiler_params=pltpu.CompilerParams(vmem_limit_bytes=2**20),
        name="write_out",
    )(*(pltpu.with_memory_space_constraint(array, pltpu.VMEM) for array in (attention, value_out)))
    return (attention[None], value_out)


def body(sizes, queries, keys_text, values_text, patch_rows, patch_owner, patch_place, value_head):
    dp_count, ctx_count, _ = sizes
    arriving = dp_count * ctx_count * patch_rows.size * patch_rows.dtype.itemsize
    arrays = (queries, keys_text, values_text, patch_rows, patch_owner, patch_place, value_head)
    if arriving > SLOT_BYTES or ctx_count % 2 or keys_text.shape[2] % (2 * HD):
        return collective_body(*arrays)
    return fused_body(sizes, *arrays)


def solution(mesh):
    in_specs = (
        P("dp", "ctx", "tp"),
        P("dp", "ctx", "tp"),
        P("dp", "ctx", "tp"),
        P("dp", "ctx", None, None, "tp"),
        P("dp", "ctx", None, None),
        P("dp", "ctx", None),
        P("tp"),
    )
    out_specs = (P("dp", "ctx", "tp"), P("dp", "ctx"))
    sizes = tuple(mesh.shape[axis] for axis in ("dp", "ctx", "tp"))
    return jax.shard_map(
        functools.partial(body, sizes),
        mesh=mesh,
        in_specs=in_specs,
        out_specs=out_specs,
        check_vma=False,
    )
```

```python
import functools
import math

import jax
import jax.numpy as jnp
from jax import lax
from jax.experimental import pallas as pl
from jax.experimental.pallas import tpu as pltpu
from jax.sharding import PartitionSpec as P

HD = 128
CAP = 4
SLOT_BYTES = 8 * 2**20
MESH = pl.DeviceIdType.MESH


def attend_block(
    carried, query_split, query_place, block_keys, block_values, key_place, score_scale
):
    running_max, denominator, numerator = carried
    scores = (
        jnp.einsum("tgrd,sgd->tgrs", query_split, block_keys, preferred_element_type=jnp.float32)
        * score_scale
    )
    allowed = (key_place[None, :] <= query_place[:, None])[:, None, None, :]
    scores = jnp.where(allowed, scores, -1e30)
    new_max = jnp.maximum(running_max, jnp.max(scores, axis=-1))
    weights = jnp.where(allowed, jnp.exp(scores - new_max[..., None]), 0.0)
    shrink = jnp.exp(running_max - new_max)
    denominator = denominator * shrink + jnp.sum(weights, axis=-1)
    numerator = numerator * shrink[..., None] + jnp.einsum(
        "tgrs,sgd->tgrd",
        weights.astype(jnp.bfloat16),
        block_values,
        preferred_element_type=jnp.float32,
    )
    return (new_max, denominator, numerator)


def unchanged(carried):
    return carried


def collective_body(queries, keys_text, values_text, patch_rows, patch_owner, patch_place, value_head):
    token_count = queries.shape[1]
    kv_width = keys_text.shape[2]
    groups = kv_width // HD
    head_count = queries.shape[2] // HD
    group_size = head_count // groups
    score_scale = HD ** (-0.5)
    dp_count = lax.axis_size("dp")
    slot_count = dp_count * CAP
    owner_seq = patch_owner[0, 0, :, 0]
    places = patch_place[0, 0]
    owner_hits = (owner_seq[:, None] == jnp.arange(dp_count, dtype=jnp.int32)[None, :]).astype(
        jnp.int32
    )
    before = jnp.cumsum(owner_hits, axis=0) - owner_hits
    slot_rank = jnp.sum(before * owner_hits, axis=1)
    target = owner_seq * CAP + slot_rank
    select = (jnp.arange(slot_count, dtype=jnp.int32)[:, None] == target[None, :]).astype(jnp.int32)
    row_data = patch_rows[0, 0].reshape(places.shape[0], 2 * kv_width)
    packed = jnp.dot(
        select.astype(jnp.bfloat16), row_data, preferred_element_type=jnp.float32
    ).astype(jnp.bfloat16)
    filled = jnp.sum(select, axis=1)
    slot_place = jnp.sum(select * places[None, :], axis=1) + (1 - filled) * token_count
    packed = packed.reshape(slot_count, 2, kv_width)
    arrived, arrived_place = (
        lax.all_to_all(packed, "dp", split_axis=0, concat_axis=0, tiled=True),
        lax.all_to_all(slot_place, "dp", split_axis=0, concat_axis=0, tiled=True),
    )
    landing = (jnp.arange(token_count, dtype=jnp.int32)[:, None] == arrived_place[None, :]).astype(
        jnp.bfloat16
    )
    arrivals = jnp.dot(
        landing, arrived.reshape(slot_count, 2 * kv_width), preferred_element_type=jnp.float32
    )
    merged_keys = (keys_text[0].astype(jnp.float32) + arrivals[:, :kv_width]).astype(jnp.bfloat16)
    merged_values = (values_text[0].astype(jnp.float32) + arrivals[:, kv_width:]).astype(
        jnp.bfloat16
    )
    query_split = queries[0].reshape(token_count, groups, group_size, HD)
    first_row = lax.axis_index("ctx") * token_count
    query_place = first_row + jnp.arange(token_count, dtype=jnp.int32)
    initial = (
        jnp.full((token_count, groups, group_size), -1e30, jnp.float32),
        jnp.zeros((token_count, groups, group_size), jnp.float32),
        jnp.zeros((token_count, groups, group_size, HD), jnp.float32),
    )
    carried = initial
    start_row = jnp.int32(0)
    piece_keys = lax.all_gather(merged_keys, "ctx", axis=0, tiled=True)
    piece_values = lax.all_gather(merged_values, "ctx", axis=0, tiled=True)
    piece_rows = piece_keys.shape[0]
    block_rows = min(512, piece_rows)
    for lower in range(0, piece_rows, block_rows):
        upper = min(lower + block_rows, piece_rows)
        block_keys = piece_keys[lower:upper].reshape(upper - lower, groups, HD)
        block_values = piece_values[lower:upper].reshape(upper - lower, groups, HD)
        key_place = start_row + lower + jnp.arange(upper - lower, dtype=jnp.int32)

        def update(state_in):
            return attend_block(
                state_in, query_split, query_place, block_keys, block_values, key_place, score_scale
            )

        carried = lax.cond(
            start_row + lower <= first_row + token_count - 1, update, unchanged, carried
        )
    running_max, denominator, numerator = carried
    attention = (
        (numerator / denominator[..., None])
        .reshape(token_count, head_count * HD)
        .astype(jnp.bfloat16)
    )
    partial_value = jnp.dot(attention, value_head, preferred_element_type=jnp.float32)
    value_out = lax.psum(partial_value, "tp")
    return (attention[None], value_out[None])


def attend(queries, merged_keys, merged_values, probe, out, last, group, totals):
    token_count, width = queries.shape
    groups = merged_keys.shape[0]
    group_size = width // HD // groups
    length = (last + 1) * token_count
    rows = token_count // len(totals)
    score_scale = HD ** (-0.5) * math.log2(math.e)
    heads = range(group * group_size, (group + 1) * group_size)
    block_keys = merged_keys[group, 0:length, :]
    summed = len(totals) > 1
    block_values = merged_values[group, 0:length, 0 : 2 * HD if summed else HD]
    for number in range(len(totals)):
        lower = number * rows
        span = slice(lower, lower + rows)
        stacked = jnp.concatenate(
            [queries[span, head * HD : (head + 1) * HD] for head in heads], axis=0
        )
        scores = lax.dot_general(
            stacked, block_keys, (((1,), (1,)), ((), ())), preferred_element_type=jnp.float32
        )
        row = lower + lax.broadcasted_iota(jnp.int32, (rows, token_count), 0)
        col = lax.broadcasted_iota(jnp.int32, (rows, token_count), 1)
        allowed = jnp.concatenate([col <= row] * group_size, axis=0)
        parts = [scores[:, j * token_count : (j + 1) * token_count] for j in range(last + 1)]
        parts[last] = jnp.where(allowed, parts[last], -1e30)
        top = jnp.max(functools.reduce(jnp.maximum, parts), axis=1, keepdims=True)
        weights = [jnp.exp2((part - top) * score_scale) for part in parts]
        rounded = jnp.concatenate([w.astype(jnp.bfloat16) for w in weights], axis=1)
        sums = jnp.dot(rounded, block_values, preferred_element_type=jnp.float32)
        if summed:
            denominator = sums[:, HD:]
        else:
            denominator = jnp.sum(functools.reduce(jnp.add, weights), axis=1, keepdims=True)
        result = (sums[:, :HD] * (1.0 / denominator)).astype(jnp.bfloat16)
        for extra, head in enumerate(heads):
            piece = result[extra * rows : (extra + 1) * rows]
            out[span, head * HD : (head + 1) * HD] = piece
            totals[number] = (
                totals[number] + piece.astype(jnp.float32) * probe[head : head + 1, :]
            )


def fused_kernel(
    sizes,
    owner_hbm,
    place_hbm,
    rows_hbm,
    keys_hbm,
    values_hbm,
    probe_hbm,
    queries_hbm,
    out_any,
    value_ref,
    queries,
    out,
    text,
    rows_in,
    spots_in,
    merged_keys,
    merged_values,
    probe_raw,
    probe,
    partial,
    partial_in,
    query_sem,
    local_sem,
    text_recv,
    patch_recv,
    value_recv,
    ready,
):
    dp_count, ctx_count, tp_count = sizes
    d, c, t = lax.axis_index("dp"), lax.axis_index("ctx"), lax.axis_index("tp")
    token_count, kv_width = keys_hbm.shape
    row_count = rows_hbm.shape[0]
    groups = kv_width // HD
    heads = queries.shape[1] // HD
    chips = ctx_count // 2
    side = lax.rem(c, 2)
    chip = c // 2
    partner = c + 1 - 2 * side

    barrier = pltpu.get_barrier_semaphore()
    in_pair = dp_count - 1

    def greet(*device):
        pl.semaphore_signal(barrier, inc=1, device_id=device, device_id_type=MESH)

    def over(lower, upper, act):
        def step(number, carry):
            act(number)
            return carry

        lax.fori_loop(lower, upper, step, 0)

    over(1, ctx_count, lambda step: greet(d, lax.rem(c + step, ctx_count), t))
    over(t + 1, tp_count, lambda other: greet(d, c, other))

    def greet_plane(there):
        for block in range(ctx_count):
            greet(there, block, t)

    over(d + 1, dp_count, greet_plane)

    def lanes(group):
        return slice(group * HD, (group + 1) * HD)

    def copy_of(src, dst, sem):
        return pltpu.make_async_copy(src, dst, sem)

    def wait_bytes(ref, sem):
        copy_of(ref, ref, sem).wait()

    patch_send, text_send, relay_send, value_send = local_sem, local_sem.at[2], local_sem.at[3], query_sem
    pass_send, out_sem = patch_recv, text_recv.at[0]
    own = c * dp_count + d
    load_patches = [
        copy_of(rows_hbm, rows_in.at[own], local_sem.at[0]),
        copy_of(owner_hbm, spots_in.at[own, 0], local_sem.at[1]),
        copy_of(place_hbm, spots_in.at[own, 1], local_sem.at[1]),
    ]
    load_probe = copy_of(probe_hbm, probe_raw, local_sem.at[2])
    load_queries = copy_of(queries_hbm, queries, query_sem.at[0])
    for load in load_patches:
        load.start()
    for group in range(groups):
        for kind, source in enumerate((keys_hbm, values_hbm)):
            copy_of(
                source.at[:, lanes(group)], text.at[c, group, kind], local_sem.at[3]
            ).start()
    load_probe.start()
    load_queries.start()
    merged_values[:, :, HD:] = jnp.ones((groups, ctx_count * token_count, HD), jnp.bfloat16)
    with jax.named_scope("w_barrier"):
        pl.semaphore_wait(barrier, d * ctx_count + ctx_count - 1 + t)

    def announce(number, *device):
        pl.semaphore_signal(
            ready.at[number], inc=1, device_id=device, device_id_type=MESH
        )

    over(
        0,
        d,
        lambda there: over(c * (1 - side), c + 1, lambda block: announce(d - 1, there, block, t)),
    )
    over(0, t, lambda other: announce(in_pair, d, c, other))
    with jax.named_scope("w_loads"):
        wait_bytes(rows_in.at[own], local_sem.at[0])
        wait_bytes(spots_in.at[own], local_sem.at[1])

    parts = (rows_in, spots_in)
    targets = chips - chip - side

    def send_patches(there, own_block):
        def to_block(block):
            for kind, part in enumerate(parts):
                pltpu.make_async_remote_copy(
                    src_ref=part.at[own],
                    dst_ref=part.at[own],
                    send_sem=patch_send.at[kind],
                    recv_sem=patch_recv.at[kind],
                    device_id=(there, block, t),
                    device_id_type=MESH,
                ).start()

        if own_block:
            to_block(c)
        over(chip + side, chips, lambda m: to_block(2 * m + 1))

    with jax.named_scope("down"):
        over(0, d, lambda there: send_patches(there, True))
    send_patches(d, False)
    with jax.named_scope("w_text"):
        wait_bytes(text.at[c], local_sem.at[3])
        load_probe.wait()
        probe[...] = probe_raw[...].astype(jnp.float32)

    def text_copy(group, block, there, sem):
        return pltpu.make_async_remote_copy(
            src_ref=text.at[block, group],
            dst_ref=text.at[block, group],
            send_sem=sem,
            recv_sem=text_recv.at[group],
            device_id=(d, there, t),
            device_id_type=MESH,
        )

    with jax.named_scope("texts"):
        for group in range(groups):
            hub = (group + 1) % 2
            over(
                chip + 1, chips, lambda m: text_copy(group, c, 2 * m + hub, text_send).start()
            )

            @pl.when(side == 0)
            def _():
                text_copy(group, c, c + 1, text_send).start()

    def send_up(there):
        pl.semaphore_wait(ready.at[there - 1], targets + 1)
        send_patches(there, True)

    def relay(last, group):
        if last:
            wait_bytes(text.at[pl.ds(0, last), group], text_recv.at[group])
        if last % 2 == (group + 1) % 2:
            for block in range(2 * (last // 2)):
                text_copy(group, block, partner, relay_send).start()

    with jax.named_scope("up"):
        over(d + 1, dp_count, send_up)
    def pass_patches(blocks):
        span = pl.ds(0, blocks * dp_count)
        for kind, part in enumerate(parts):
            pltpu.make_async_remote_copy(
                src_ref=part.at[span],
                dst_ref=part.at[span],
                send_sem=pass_send.at[kind],
                recv_sem=patch_recv.at[kind],
                device_id=(d, c - 1, t),
                device_id_type=MESH,
            ).start()

    def merge(block, chosen):
        slots = dp_count * row_count
        span = slice(block * dp_count, (block + 1) * dp_count)
        spots = spots_in[span]
        code = spots[:, 0] * token_count + spots[:, 1]
        code = jnp.concatenate([code[k] for k in range(dp_count)], axis=1)
        here = d * token_count + lax.broadcasted_iota(jnp.int32, (token_count, slots), 0)
        landing = jnp.where(code == here, 1.0, 0.0).astype(jnp.bfloat16)
        wide = slice(chosen[0] * HD, (chosen[-1] + 1) * HD)
        rows = rows_in[span, :, :, wide].astype(jnp.float32)
        tokens = slice(block * token_count, (block + 1) * token_count)
        for kind in range(2):
            kind_rows = rows[:, :, kind, :].reshape(slots, -1).astype(jnp.bfloat16)
            arrivals = jnp.dot(landing, kind_rows, preferred_element_type=jnp.float32)
            for number, group in enumerate(chosen):
                whole = text[block, group, kind].astype(jnp.float32) + arrivals[:, lanes(number)]
                if kind == 0:
                    merged_keys[group, tokens, :] = whole.astype(jnp.bfloat16)
                else:
                    merged_values[group, tokens, 0:HD] = whole.astype(jnp.bfloat16)

    def finish(last):
        hubs = [group for group in range(groups) if last % 2 == (group + 1) % 2]
        others = [group for group in range(groups) if group not in hubs]
        with jax.named_scope("relay"):
            for group in hubs:
                relay(last, group)
        with jax.named_scope("w_patch"):
            for kind, part in enumerate(parts):
                wait_bytes(part.at[pl.ds(0, (last + 1) * dp_count - 1)], patch_recv.at[kind])
            if last % 2 and last > 1:
                pass_patches(last - 1)
        with jax.named_scope("w_kv"):
            for group in others:
                relay(last, group)
            load_queries.wait()
        with jax.named_scope("attend"):
            rows = math.gcd(token_count, 16) if last % 2 and last > 1 else token_count
            totals = [jnp.zeros((rows, HD), jnp.float32)] * (token_count // rows)
            for block in range(last + 1):
                merge(block, range(groups))
            for group in range(groups):
                attend(queries, merged_keys, merged_values, probe, out, last, group, totals)
        total = jnp.concatenate(totals, axis=0)
        partial[...] = jnp.sum(jnp.transpose(total), axis=0, keepdims=True)

    for last in range(ctx_count):

        @pl.when(c == last)
        def _():
            finish(last)

    value_copies = [
        pltpu.make_async_remote_copy(
            src_ref=partial,
            dst_ref=partial_in.at[k - 1],
            send_sem=value_send.at[k - 1],
            recv_sem=value_recv.at[k - 1],
            device_id=(d, c, lax.rem(t + k, tp_count)),
            device_id_type=MESH,
        )
        for k in range(1, tp_count)
    ]
    with jax.named_scope("w_pair"):

        @pl.when(t < tp_count - 1)
        def _():
            pl.semaphore_wait(ready.at[in_pair], tp_count - 1 - t)

    for copy in value_copies:
        copy.start()
    store = copy_of(out, out_any, out_sem)
    store.start()
    with jax.named_scope("tail"):
        for last in range(ctx_count):

            @pl.when(c == last)
            def _():
                sent = dp_count * (chips - last // 2 - last % 2 + 1) - 1
                for kind, part in enumerate(parts):
                    if sent:
                        wait_bytes(part.at[pl.ds(0, sent)], patch_send.at[kind])
                    if last % 2 and last > 1:
                        wait_bytes(part.at[pl.ds(0, (last - 1) * dp_count)], pass_send.at[kind])
                copies = chips - last // 2 - last % 2
                if copies:
                    wait_bytes(text.at[pl.ds(0, copies)], text_send)
                relayed = 2 * (last // 2) * len([h for h in range(groups) if last % 2 == (h + 1) % 2])
                if relayed:
                    wait_bytes(text.at[pl.ds(0, relayed // groups)], relay_send)

        store.wait()
        for copy in value_copies:
            copy.wait()
    whole = partial[...]
    for k in range(1, tp_count):
        whole = whole + partial_in[k - 1]
    value_ref[...] = whole


def write_kernel(attention, value, attention_hbm, value_hbm, sems):
    pieces = sems.shape[0] - 1
    rows = attention.shape[0] // pieces
    copies = [pltpu.make_async_copy(value, value_hbm, sems.at[pieces])]
    for number in range(pieces):
        span = pl.ds(number * rows, rows)
        copies.append(
            pltpu.make_async_copy(
                attention.at[span, :], attention_hbm.at[span, :], sems.at[number]
            )
        )
    for copy in copies:
        copy.start()
    for copy in copies:
        copy.wait()


def fused_body(sizes, queries, keys_text, values_text, patch_rows, patch_owner, patch_place, value_head):
    dp_count, ctx_count, tp_count = sizes
    _, token_count, query_width = queries.shape
    kv_width = keys_text.shape[2]
    row_count = patch_rows.shape[2]
    heads = query_width // HD
    groups = kv_width // HD
    dma = pltpu.SemaphoreType.DMA
    vmem = pl.BlockSpec(memory_space=pltpu.VMEM)
    anywhere = pl.BlockSpec(memory_space=pl.ANY)
    others = max(tp_count - 1, 1)
    inputs = (
        patch_owner[0, 0].reshape(1, row_count),
        patch_place[0],
        patch_rows[0, 0],
        keys_text[0],
        values_text[0],
        value_head.reshape(heads, HD),
        queries[0],
    )
    shapes = (
        jax.ShapeDtypeStruct((token_count, query_width), jnp.bfloat16),
        jax.ShapeDtypeStruct((1, token_count), jnp.float32),
    )
    attention, value_out = pl.pallas_call(
        functools.partial(fused_kernel, sizes),
        out_shape=shapes,
        in_specs=[pl.BlockSpec(memory_space=pltpu.HBM)] * 7,
        out_specs=(anywhere, vmem),
        scratch_shapes=[
            pltpu.VMEM((token_count, query_width), jnp.bfloat16),
            pltpu.VMEM((token_count, query_width), jnp.bfloat16),
            pltpu.VMEM((ctx_count, groups, 2, token_count, HD), jnp.bfloat16),
            pltpu.VMEM((ctx_count * dp_count, row_count, 2, kv_width), jnp.bfloat16),
            pltpu.VMEM((ctx_count * dp_count, 2, 1, row_count), jnp.int32),
            pltpu.VMEM((groups, ctx_count * token_count, HD), jnp.bfloat16),
            pltpu.VMEM((groups, ctx_count * token_count, 2 * HD), jnp.bfloat16),
            pltpu.VMEM((heads, HD), jnp.bfloat16),
            pltpu.VMEM((heads, HD), jnp.float32),
            pltpu.VMEM((1, token_count), jnp.float32),
            pltpu.VMEM((others, 1, token_count), jnp.float32),
            dma((others,)),
            dma((4,)),
            dma((groups,)),
            dma((2,)),
            dma((others,)),
            pltpu.SemaphoreType.REGULAR((dp_count,)),
        ],
        compiler_params=pltpu.CompilerParams(
            collective_id=0, has_side_effects=True, vmem_limit_bytes=24 * 2**20
        ),
        name="merged_attention",
    )(*(pltpu.with_memory_space_constraint(array, pltpu.HBM) for array in inputs))
    attention, value_out = pl.pallas_call(
        write_kernel,
        out_shape=shapes,
        in_specs=[anywhere] * 2,
        out_specs=(pl.BlockSpec(memory_space=pltpu.HBM),) * 2,
        scratch_shapes=[dma((2,))],
        compiler_params=pltpu.CompilerParams(vmem_limit_bytes=2**20),
        name="write_out",
    )(*(pltpu.with_memory_space_constraint(array, pltpu.VMEM) for array in (attention, value_out)))
    return (attention[None], value_out)


def body(sizes, queries, keys_text, values_text, patch_rows, patch_owner, patch_place, value_head):
    dp_count, ctx_count, _ = sizes
    arriving = dp_count * ctx_count * patch_rows.size * patch_rows.dtype.itemsize
    arrays = (queries, keys_text, values_text, patch_rows, patch_owner, patch_place, value_head)
    if arriving > SLOT_BYTES or ctx_count % 2 or keys_text.shape[2] % (2 * HD):
        return collective_body(*arrays)
    return fused_body(sizes, *arrays)


def solution(mesh):
    in_specs = (
        P("dp", "ctx", "tp"),
        P("dp", "ctx", "tp"),
        P("dp", "ctx", "tp"),
        P("dp", "ctx", None, None, "tp"),
        P("dp", "ctx", None, None),
        P("dp", "ctx", None),
        P("tp"),
    )
    out_specs = (P("dp", "ctx", "tp"), P("dp", "ctx"))
    sizes = tuple(mesh.shape[axis] for axis in ("dp", "ctx", "tp"))
    return jax.shard_map(
        functools.partial(body, sizes),
        mesh=mesh,
        in_specs=in_specs,
        out_specs=out_specs,
        check_vma=False,
    )
```

```python
import functools
import math

import jax
import jax.numpy as jnp
from jax import lax
from jax.experimental import pallas as pl
from jax.experimental.pallas import tpu as pltpu
from jax.sharding import PartitionSpec as P

HD = 128
CAP = 4
SLOT_BYTES = 8 * 2**20
MESH = pl.DeviceIdType.MESH


def attend_block(
    carried, query_split, query_place, block_keys, block_values, key_place, score_scale
):
    running_max, denominator, numerator = carried
    scores = (
        jnp.einsum("tgrd,sgd->tgrs", query_split, block_keys, preferred_element_type=jnp.float32)
        * score_scale
    )
    allowed = (key_place[None, :] <= query_place[:, None])[:, None, None, :]
    scores = jnp.where(allowed, scores, -1e30)
    new_max = jnp.maximum(running_max, jnp.max(scores, axis=-1))
    weights = jnp.where(allowed, jnp.exp(scores - new_max[..., None]), 0.0)
    shrink = jnp.exp(running_max - new_max)
    denominator = denominator * shrink + jnp.sum(weights, axis=-1)
    numerator = numerator * shrink[..., None] + jnp.einsum(
        "tgrs,sgd->tgrd",
        weights.astype(jnp.bfloat16),
        block_values,
        preferred_element_type=jnp.float32,
    )
    return (new_max, denominator, numerator)


def unchanged(carried):
    return carried


def collective_body(queries, keys_text, values_text, patch_rows, patch_owner, patch_place, value_head):
    token_count = queries.shape[1]
    kv_width = keys_text.shape[2]
    groups = kv_width // HD
    head_count = queries.shape[2] // HD
    group_size = head_count // groups
    score_scale = HD ** (-0.5)
    dp_count = lax.axis_size("dp")
    slot_count = dp_count * CAP
    owner_seq = patch_owner[0, 0, :, 0]
    places = patch_place[0, 0]
    owner_hits = (owner_seq[:, None] == jnp.arange(dp_count, dtype=jnp.int32)[None, :]).astype(
        jnp.int32
    )
    before = jnp.cumsum(owner_hits, axis=0) - owner_hits
    slot_rank = jnp.sum(before * owner_hits, axis=1)
    target = owner_seq * CAP + slot_rank
    select = (jnp.arange(slot_count, dtype=jnp.int32)[:, None] == target[None, :]).astype(jnp.int32)
    row_data = patch_rows[0, 0].reshape(places.shape[0], 2 * kv_width)
    packed = jnp.dot(
        select.astype(jnp.bfloat16), row_data, preferred_element_type=jnp.float32
    ).astype(jnp.bfloat16)
    filled = jnp.sum(select, axis=1)
    slot_place = jnp.sum(select * places[None, :], axis=1) + (1 - filled) * token_count
    packed = packed.reshape(slot_count, 2, kv_width)
    arrived, arrived_place = (
        lax.all_to_all(packed, "dp", split_axis=0, concat_axis=0, tiled=True),
        lax.all_to_all(slot_place, "dp", split_axis=0, concat_axis=0, tiled=True),
    )
    landing = (jnp.arange(token_count, dtype=jnp.int32)[:, None] == arrived_place[None, :]).astype(
        jnp.bfloat16
    )
    arrivals = jnp.dot(
        landing, arrived.reshape(slot_count, 2 * kv_width), preferred_element_type=jnp.float32
    )
    merged_keys = (keys_text[0].astype(jnp.float32) + arrivals[:, :kv_width]).astype(jnp.bfloat16)
    merged_values = (values_text[0].astype(jnp.float32) + arrivals[:, kv_width:]).astype(
        jnp.bfloat16
    )
    query_split = queries[0].reshape(token_count, groups, group_size, HD)
    first_row = lax.axis_index("ctx") * token_count
    query_place = first_row + jnp.arange(token_count, dtype=jnp.int32)
    initial = (
        jnp.full((token_count, groups, group_size), -1e30, jnp.float32),
        jnp.zeros((token_count, groups, group_size), jnp.float32),
        jnp.zeros((token_count, groups, group_size, HD), jnp.float32),
    )
    carried = initial
    start_row = jnp.int32(0)
    piece_keys = lax.all_gather(merged_keys, "ctx", axis=0, tiled=True)
    piece_values = lax.all_gather(merged_values, "ctx", axis=0, tiled=True)
    piece_rows = piece_keys.shape[0]
    block_rows = min(512, piece_rows)
    for lower in range(0, piece_rows, block_rows):
        upper = min(lower + block_rows, piece_rows)
        block_keys = piece_keys[lower:upper].reshape(upper - lower, groups, HD)
        block_values = piece_values[lower:upper].reshape(upper - lower, groups, HD)
        key_place = start_row + lower + jnp.arange(upper - lower, dtype=jnp.int32)

        def update(state_in):
            return attend_block(
                state_in, query_split, query_place, block_keys, block_values, key_place, score_scale
            )

        carried = lax.cond(
            start_row + lower <= first_row + token_count - 1, update, unchanged, carried
        )
    running_max, denominator, numerator = carried
    attention = (
        (numerator / denominator[..., None])
        .reshape(token_count, head_count * HD)
        .astype(jnp.bfloat16)
    )
    partial_value = jnp.dot(attention, value_head, preferred_element_type=jnp.float32)
    value_out = lax.psum(partial_value, "tp")
    return (attention[None], value_out[None])


def attend(queries, merged_keys, merged_values, probe, out, last, group, totals):
    token_count, width = queries.shape
    groups = merged_keys.shape[0]
    group_size = width // HD // groups
    length = (last + 1) * token_count
    rows = token_count // len(totals)
    score_scale = HD ** (-0.5) * math.log2(math.e)
    heads = range(group * group_size, (group + 1) * group_size)
    block_keys = merged_keys[group, 0:length, :]
    summed = len(totals) > 1
    block_values = merged_values[group, 0:length, 0 : 2 * HD if summed else HD]
    for number in range(len(totals)):
        lower = number * rows
        span = slice(lower, lower + rows)
        stacked = jnp.concatenate(
            [queries[span, head * HD : (head + 1) * HD] for head in heads], axis=0
        )
        scores = lax.dot_general(
            stacked, block_keys, (((1,), (1,)), ((), ())), preferred_element_type=jnp.float32
        )
        row = lower + lax.broadcasted_iota(jnp.int32, (rows, token_count), 0)
        col = lax.broadcasted_iota(jnp.int32, (rows, token_count), 1)
        allowed = jnp.concatenate([col <= row] * group_size, axis=0)
        parts = [scores[:, j * token_count : (j + 1) * token_count] for j in range(last + 1)]
        parts[last] = jnp.where(allowed, parts[last], -1e30)
        top = jnp.max(functools.reduce(jnp.maximum, parts), axis=1, keepdims=True)
        weights = [jnp.exp2((part - top) * score_scale) for part in parts]
        rounded = jnp.concatenate([w.astype(jnp.bfloat16) for w in weights], axis=1)
        sums = jnp.dot(rounded, block_values, preferred_element_type=jnp.float32)
        if summed:
            denominator = sums[:, HD:]
        else:
            denominator = jnp.sum(functools.reduce(jnp.add, weights), axis=1, keepdims=True)
        result = (sums[:, :HD] * (1.0 / denominator)).astype(jnp.bfloat16)
        for extra, head in enumerate(heads):
            piece = result[extra * rows : (extra + 1) * rows]
            out[span, head * HD : (head + 1) * HD] = piece
            totals[number] = (
                totals[number] + piece.astype(jnp.float32) * probe[head : head + 1, :]
            )


def fused_kernel(
    sizes,
    owner_hbm,
    place_hbm,
    rows_hbm,
    keys_hbm,
    values_hbm,
    probe_hbm,
    queries_hbm,
    out_any,
    value_ref,
    queries,
    out,
    text,
    rows_in,
    spots_in,
    merged_keys,
    merged_values,
    probe_raw,
    probe,
    partial,
    partial_in,
    query_sem,
    local_sem,
    text_recv,
    patch_recv,
    value_recv,
    ready,
):
    dp_count, ctx_count, tp_count = sizes
    d, c, t = lax.axis_index("dp"), lax.axis_index("ctx"), lax.axis_index("tp")
    token_count, kv_width = keys_hbm.shape
    row_count = rows_hbm.shape[0]
    groups = kv_width // HD
    heads = queries.shape[1] // HD
    chips = ctx_count // 2
    side = lax.rem(c, 2)
    chip = c // 2
    partner = c + 1 - 2 * side

    barrier = pltpu.get_barrier_semaphore()
    in_pair = dp_count - 1

    def greet(*device):
        pl.semaphore_signal(barrier, inc=1, device_id=device, device_id_type=MESH)

    def over(lower, upper, act):
        def step(number, carry):
            act(number)
            return carry

        lax.fori_loop(lower, upper, step, 0)

    over(1, ctx_count, lambda step: greet(d, lax.rem(c + step, ctx_count), t))
    over(t + 1, tp_count, lambda other: greet(d, c, other))

    def greet_plane(there):
        for block in range(ctx_count):
            greet(there, block, t)

    over(d + 1, dp_count, greet_plane)

    def lanes(group):
        return slice(group * HD, (group + 1) * HD)

    def copy_of(src, dst, sem):
        return pltpu.make_async_copy(src, dst, sem)

    def wait_bytes(ref, sem):
        copy_of(ref, ref, sem).wait()

    patch_send, text_send, relay_send, value_send = local_sem, local_sem.at[2], local_sem.at[3], query_sem
    pass_send, out_sem = patch_recv, text_recv.at[0]
    own = c * dp_count + d
    load_patches = [
        copy_of(rows_hbm, rows_in.at[own], local_sem.at[0]),
        copy_of(owner_hbm, spots_in.at[own, 0], local_sem.at[1]),
        copy_of(place_hbm, spots_in.at[own, 1], local_sem.at[1]),
    ]
    load_probe = copy_of(probe_hbm, probe_raw, local_sem.at[2])
    load_queries = copy_of(queries_hbm, queries, query_sem.at[0])
    for load in load_patches:
        load.start()
    for group in range(groups):
        for kind, source in enumerate((keys_hbm, values_hbm)):
            copy_of(
                source.at[:, lanes(group)], text.at[c, group, kind], local_sem.at[3]
            ).start()
    load_probe.start()
    load_queries.start()

    @pl.when((side == 1) & (chip > 0))
    def _():
        merged_values[:, :, HD:] = jnp.ones((groups, ctx_count * token_count, HD), jnp.bfloat16)

    with jax.named_scope("w_barrier"):
        pl.semaphore_wait(barrier, d * ctx_count + ctx_count - 1 + t)

    def announce(number, *device):
        pl.semaphore_signal(
            ready.at[number], inc=1, device_id=device, device_id_type=MESH
        )

    over(
        0,
        d,
        lambda there: over(c * (1 - side), c + 1, lambda block: announce(d - 1, there, block, t)),
    )
    over(0, t, lambda other: announce(in_pair, d, c, other))
    with jax.named_scope("w_loads"):
        wait_bytes(rows_in.at[own], local_sem.at[0])
        wait_bytes(spots_in.at[own], local_sem.at[1])

    parts = (rows_in, spots_in)
    targets = chips - chip - side

    def send_patches(there, own_block):
        def to_block(block):
            for kind, part in enumerate(parts):
                pltpu.make_async_remote_copy(
                    src_ref=part.at[own],
                    dst_ref=part.at[own],
                    send_sem=patch_send.at[kind],
                    recv_sem=patch_recv.at[kind],
                    device_id=(there, block, t),
                    device_id_type=MESH,
                ).start()

        if own_block:
            to_block(c)
        over(chip + side, chips, lambda m: to_block(2 * m + 1))

    with jax.named_scope("down"):
        over(0, d, lambda there: send_patches(there, True))
    send_patches(d, False)
    with jax.named_scope("w_text"):
        wait_bytes(text.at[c], local_sem.at[3])
        load_probe.wait()
        probe[...] = probe_raw[...].astype(jnp.float32)

    def text_copy(group, block, there, sem):
        return pltpu.make_async_remote_copy(
            src_ref=text.at[block, group],
            dst_ref=text.at[block, group],
            send_sem=sem,
            recv_sem=text_recv.at[group],
            device_id=(d, there, t),
            device_id_type=MESH,
        )

    with jax.named_scope("texts"):
        for group in range(groups):
            hub = (group + 1) % 2
            over(
                chip + 1, chips, lambda m: text_copy(group, c, 2 * m + hub, text_send).start()
            )

            @pl.when(side == 0)
            def _():
                text_copy(group, c, c + 1, text_send).start()

    def send_up(there):
        pl.semaphore_wait(ready.at[there - 1], targets + 1)
        send_patches(there, True)

    def relay(last, group):
        if last:
            wait_bytes(text.at[pl.ds(0, last), group], text_recv.at[group])
        if last % 2 == (group + 1) % 2:
            for block in range(2 * (last // 2)):
                text_copy(group, block, partner, relay_send).start()

    with jax.named_scope("up"):
        over(d + 1, dp_count, send_up)
    def pass_patches(blocks):
        span = pl.ds(0, blocks * dp_count)
        for kind, part in enumerate(parts):
            pltpu.make_async_remote_copy(
                src_ref=part.at[span],
                dst_ref=part.at[span],
                send_sem=pass_send.at[kind],
                recv_sem=patch_recv.at[kind],
                device_id=(d, c - 1, t),
                device_id_type=MESH,
            ).start()

    def merge(block, chosen):
        slots = dp_count * row_count
        span = slice(block * dp_count, (block + 1) * dp_count)
        spots = spots_in[span]
        code = spots[:, 0] * token_count + spots[:, 1]
        code = jnp.concatenate([code[k] for k in range(dp_count)], axis=1)
        here = d * token_count + lax.broadcasted_iota(jnp.int32, (token_count, slots), 0)
        landing = jnp.where(code == here, 1.0, 0.0).astype(jnp.bfloat16)
        wide = slice(chosen[0] * HD, (chosen[-1] + 1) * HD)
        rows = rows_in[span, :, :, wide].astype(jnp.float32)
        tokens = slice(block * token_count, (block + 1) * token_count)
        for kind in range(2):
            kind_rows = rows[:, :, kind, :].reshape(slots, -1).astype(jnp.bfloat16)
            arrivals = jnp.dot(landing, kind_rows, preferred_element_type=jnp.float32)
            for number, group in enumerate(chosen):
                whole = text[block, group, kind].astype(jnp.float32) + arrivals[:, lanes(number)]
                if kind == 0:
                    merged_keys[group, tokens, :] = whole.astype(jnp.bfloat16)
                else:
                    merged_values[group, tokens, 0:HD] = whole.astype(jnp.bfloat16)

    def finish(last):
        hubs = [group for group in range(groups) if last % 2 == (group + 1) % 2]
        others = [group for group in range(groups) if group not in hubs]
        with jax.named_scope("relay"):
            for group in hubs:
                relay(last, group)
        with jax.named_scope("w_patch"):
            for kind, part in enumerate(parts):
                wait_bytes(part.at[pl.ds(0, (last + 1) * dp_count - 1)], patch_recv.at[kind])
            if last % 2 and last > 1:
                pass_patches(last - 1)
        with jax.named_scope("w_kv"):
            for group in others:
                relay(last, group)
            load_queries.wait()
        with jax.named_scope("attend"):
            rows = math.gcd(token_count, 16) if last % 2 and last > 1 else token_count
            totals = [jnp.zeros((rows, HD), jnp.float32)] * (token_count // rows)
            for block in range(last + 1):
                merge(block, range(groups))
            for group in range(groups):
                attend(queries, merged_keys, merged_values, probe, out, last, group, totals)
        total = jnp.concatenate(totals, axis=0)
        partial[...] = jnp.sum(jnp.transpose(total), axis=0, keepdims=True)

    for last in range(ctx_count):

        @pl.when(c == last)
        def _():
            finish(last)

    value_copies = [
        pltpu.make_async_remote_copy(
            src_ref=partial,
            dst_ref=partial_in.at[k - 1],
            send_sem=value_send.at[k - 1],
            recv_sem=value_recv.at[k - 1],
            device_id=(d, c, lax.rem(t + k, tp_count)),
            device_id_type=MESH,
        )
        for k in range(1, tp_count)
    ]
    with jax.named_scope("w_pair"):

        @pl.when(t < tp_count - 1)
        def _():
            pl.semaphore_wait(ready.at[in_pair], tp_count - 1 - t)

    for copy in value_copies:
        copy.start()
    store = copy_of(out, out_any, out_sem)
    store.start()
    with jax.named_scope("tail"):
        for last in range(ctx_count):

            @pl.when(c == last)
            def _():
                sent = dp_count * (chips - last // 2 - last % 2 + 1) - 1
                for kind, part in enumerate(parts):
                    if sent:
                        wait_bytes(part.at[pl.ds(0, sent)], patch_send.at[kind])
                    if last % 2 and last > 1:
                        wait_bytes(part.at[pl.ds(0, (last - 1) * dp_count)], pass_send.at[kind])
                copies = chips - last // 2 - last % 2
                if copies:
                    wait_bytes(text.at[pl.ds(0, copies)], text_send)
                relayed = 2 * (last // 2) * len([h for h in range(groups) if last % 2 == (h + 1) % 2])
                if relayed:
                    wait_bytes(text.at[pl.ds(0, relayed // groups)], relay_send)

        store.wait()
        for copy in value_copies:
            copy.wait()
    whole = partial[...]
    for k in range(1, tp_count):
        whole = whole + partial_in[k - 1]
    value_ref[...] = whole


def write_kernel(attention, value, attention_hbm, value_hbm, sems):
    pieces = sems.shape[0] - 1
    rows = attention.shape[0] // pieces
    copies = [pltpu.make_async_copy(value, value_hbm, sems.at[pieces])]
    for number in range(pieces):
        span = pl.ds(number * rows, rows)
        copies.append(
            pltpu.make_async_copy(
                attention.at[span, :], attention_hbm.at[span, :], sems.at[number]
            )
        )
    for copy in copies:
        copy.start()
    for copy in copies:
        copy.wait()


def fused_body(sizes, queries, keys_text, values_text, patch_rows, patch_owner, patch_place, value_head):
    dp_count, ctx_count, tp_count = sizes
    _, token_count, query_width = queries.shape
    kv_width = keys_text.shape[2]
    row_count = patch_rows.shape[2]
    heads = query_width // HD
    groups = kv_width // HD
    dma = pltpu.SemaphoreType.DMA
    vmem = pl.BlockSpec(memory_space=pltpu.VMEM)
    anywhere = pl.BlockSpec(memory_space=pl.ANY)
    others = max(tp_count - 1, 1)
    inputs = (
        patch_owner[0, 0].reshape(1, row_count),
        patch_place[0],
        patch_rows[0, 0],
        keys_text[0],
        values_text[0],
        value_head.reshape(heads, HD),
        queries[0],
    )
    shapes = (
        jax.ShapeDtypeStruct((token_count, query_width), jnp.bfloat16),
        jax.ShapeDtypeStruct((1, token_count), jnp.float32),
    )
    attention, value_out = pl.pallas_call(
        functools.partial(fused_kernel, sizes),
        out_shape=shapes,
        in_specs=[pl.BlockSpec(memory_space=pltpu.HBM)] * 7,
        out_specs=(anywhere, vmem),
        scratch_shapes=[
            pltpu.VMEM((token_count, query_width), jnp.bfloat16),
            pltpu.VMEM((token_count, query_width), jnp.bfloat16),
            pltpu.VMEM((ctx_count, groups, 2, token_count, HD), jnp.bfloat16),
            pltpu.VMEM((ctx_count * dp_count, row_count, 2, kv_width), jnp.bfloat16),
            pltpu.VMEM((ctx_count * dp_count, 2, 1, row_count), jnp.int32),
            pltpu.VMEM((groups, ctx_count * token_count, HD), jnp.bfloat16),
            pltpu.VMEM((groups, ctx_count * token_count, 2 * HD), jnp.bfloat16),
            pltpu.VMEM((heads, HD), jnp.bfloat16),
            pltpu.VMEM((heads, HD), jnp.float32),
            pltpu.VMEM((1, token_count), jnp.float32),
            pltpu.VMEM((others, 1, token_count), jnp.float32),
            dma((others,)),
            dma((4,)),
            dma((groups,)),
            dma((2,)),
            dma((others,)),
            pltpu.SemaphoreType.REGULAR((dp_count,)),
        ],
        compiler_params=pltpu.CompilerParams(
            collective_id=0, has_side_effects=True, vmem_limit_bytes=24 * 2**20
        ),
        name="merged_attention",
    )(*(pltpu.with_memory_space_constraint(array, pltpu.HBM) for array in inputs))
    attention, value_out = pl.pallas_call(
        write_kernel,
        out_shape=shapes,
        in_specs=[anywhere] * 2,
        out_specs=(pl.BlockSpec(memory_space=pltpu.HBM),) * 2,
        scratch_shapes=[dma((2,))],
        compiler_params=pltpu.CompilerParams(vmem_limit_bytes=2**20),
        name="write_out",
    )(*(pltpu.with_memory_space_constraint(array, pltpu.VMEM) for array in (attention, value_out)))
    return (attention[None], value_out)


def body(sizes, queries, keys_text, values_text, patch_rows, patch_owner, patch_place, value_head):
    dp_count, ctx_count, _ = sizes
    arriving = dp_count * ctx_count * patch_rows.size * patch_rows.dtype.itemsize
    arrays = (queries, keys_text, values_text, patch_rows, patch_owner, patch_place, value_head)
    if arriving > SLOT_BYTES or ctx_count % 2 or keys_text.shape[2] % (2 * HD):
        return collective_body(*arrays)
    return fused_body(sizes, *arrays)


def solution(mesh):
    in_specs = (
        P("dp", "ctx", "tp"),
        P("dp", "ctx", "tp"),
        P("dp", "ctx", "tp"),
        P("dp", "ctx", None, None, "tp"),
        P("dp", "ctx", None, None),
        P("dp", "ctx", None),
        P("tp"),
    )
    out_specs = (P("dp", "ctx", "tp"), P("dp", "ctx"))
    sizes = tuple(mesh.shape[axis] for axis in ("dp", "ctx", "tp"))
    return jax.shard_map(
        functools.partial(body, sizes),
        mesh=mesh,
        in_specs=in_specs,
        out_specs=out_specs,
        check_vma=False,
    )
```
